32 devices in a mesh: row: 8 (over y, x, core), col: 4 (over z).
Axes of the slice: x: 2, y: 2, z: 4, core: 2. Of those that a mesh axis runs over, the one named last changes fastest.
Arguments:
- state: float32 [9, 35, 8192], P(None, None, ('col', 'row')), may hold values from -6 to 6
- geometry: bfloat16 [9, 128, 8192], P(None, 'row', 'col'), may hold values from -5 to 5
- material: float32 [4, 8192], P(None, ('col', 'row')), may hold values from 0.5 to 2
- neighbours: int32 [4, 4, 8192], P(None, None, ('col', 'row')), may hold values from 0 to 1023, as said below
- send_faces: int32 [32, 4, 64], P(('col', 'row')), may hold values from 0 to 1023, as said below
- vol_eval: float32 [35, 128], replicated, may hold values from -1 to 1
- vol_grad: bfloat16 [3, 35, 128], replicated, may hold values from -0.3125 to 0.3125
- face_eval: float32 [4, 35, 27], replicated, may hold values from -1 to 1
- face_lift: float32 [4, 35, 27], replicated, may hold values from -0.625 to 0.625
- normals: bfloat16 [3, 27, 4, 8192], P(None, None, None, ('col', 'row')), may hold values from -5 to 5
- areas: float32 [27, 4, 8192], P(None, None, ('col', 'row')), may hold values from 0.5 to 2
Outputs:
- section: float32 [9, 35, 8192], P(None, None, ('col', 'row'))
The draws below stay inside these ranges and needn't reach their ends.
Inputs may be any that keep to these rules, and one draw needn't show every extreme that they name: `neighbours`: field 0 is the kind: 0 the neighbour face lies in the same block, 1 in another block of the same row group, 2 free surface, 3 absorbing. Field 1 is the neighbour block's col index (the own col index for kinds 0, 2, 3). Field 2 is, for kind 0, the neighbour's face number f * 256 + e within the block; for kind 1, a slot below the number of faces that the neighbour's block lists for this block in send_faces; else 0. Field 3 is an orientation of 0 to 2 (0 for kinds 2 and 3). Neighbouring is mutual: the neighbour face names this face back, with orientation (3 - turn) % 3. `send_faces`: A block lists at most 64 faces for one col index, the same number as that block lists back, and nothing for its own col index; entries past the count are 0. In every row group some pair of blocks lists exactly 64 faces to each other.
All inputs are finite; a program needn't handle non-finite values.
Results may differ from the reference program's by a relative error of at most 0.0065.
Values may be sent and summed in bfloat16 or wider, within the bound.
A program may use at most 64 MiB of HBM per device.

```python
import math
import jax
import jax.numpy as jnp
from jax import lax

NQ = 9
NB = 35
VQ = 128
FQ = 27
E_DEV = 256
SLOTS = 64
ELEMENTS = 8192
N_ROW = 8
N_COL = 4


def build_faces(key):
    face_count = 4 * E_DEV
    column_ids = jnp.arange(N_COL, dtype=jnp.int32)
    upper_half = column_ids[:, None] < column_ids[None, :]
    counts = jax.random.randint(jax.random.fold_in(key, 11), (N_ROW, N_COL, N_COL), SLOTS // 4, SLOTS + 1)
    counts = jnp.where(upper_half[None], counts, jnp.transpose(counts, (0, 2, 1)))
    first_col = jax.random.randint(jax.random.fold_in(key, 12), (N_ROW, 1, 1), 0, N_COL)
    second_col = (first_col + jax.random.randint(jax.random.fold_in(key, 13), (N_ROW, 1, 1), 1, N_COL)) % N_COL
    sender = column_ids[None, :, None]
    getter = column_ids[None, None, :]
    filled = (sender == first_col) & (getter == second_col) | (sender == second_col) & (getter == first_col)
    counts = jnp.where(filled, SLOTS, counts)
    counts = jnp.where(sender == getter, 0, counts).astype(jnp.int32)
    pair_turns = jax.random.randint(jax.random.fold_in(key, 14), (N_ROW, N_COL, N_COL, SLOTS), 0, 3)
    pair_turns = jnp.where(upper_half[None, :, :, None], pair_turns, (3 - jnp.transpose(pair_turns, (0, 2, 1, 3))) % 3)

    def one_device(row_id, column_id):
        device_key = jax.random.fold_in(jax.random.fold_in(key, 15), column_id * N_ROW + row_id)
        shuffle = jax.random.permutation(jax.random.fold_in(device_key, 1), face_count).astype(jnp.int32)
        own_counts = counts[row_id, column_id]
        list_ends = jnp.cumsum(own_counts)
        starts = list_ends - own_counts
        remote_total = list_ends[N_COL - 1]
        positions = jnp.arange(face_count, dtype=jnp.int32)
        peer_index = jnp.minimum(jnp.sum((list_ends[None, :] <= positions[:, None]).astype(jnp.int32), axis=1), N_COL - 1)
        slot_index = jnp.clip(positions - starts[peer_index], 0, SLOTS - 1)
        remote = positions < remote_total
        offset = positions - remote_total
        remaining = face_count - remote_total
        edge_total = jax.random.randint(jax.random.fold_in(device_key, 2), (), face_count // 16, face_count // 8 + 1)
        paired = 2 * ((remaining - edge_total) // 2)
        is_pair = (offset >= 0) & (offset < paired)
        partner = jnp.clip(remote_total + jnp.bitwise_xor(jnp.maximum(offset, 0), 1), 0, face_count - 1)
        local_turns = jax.random.randint(jax.random.fold_in(device_key, 3), (face_count,), 0, 3)
        base_turn = local_turns[jnp.clip(remote_total + offset - offset % 2, 0, face_count - 1)]
        pair_turn = jnp.where(offset % 2 == 0, base_turn, (3 - base_turn) % 3)
        edge_kind = 2 + jax.random.randint(jax.random.fold_in(device_key, 4), (face_count,), 0, 2)
        face_kind = jnp.where(remote, 1, jnp.where(is_pair, 0, edge_kind))
        peer_field = jnp.where(remote, peer_index, column_id)
        target = jnp.where(remote, slot_index, jnp.where(is_pair, shuffle[partner], 0))
        turning = jnp.where(remote, pair_turns[row_id, column_id, peer_index, slot_index], jnp.where(is_pair, pair_turn, 0))
        fields = jnp.stack([face_kind, peer_field, target, turning]).astype(jnp.int32)
        by_face = jnp.zeros((4, face_count), jnp.int32).at[:, shuffle].set(fields)
        slot_ids = jnp.arange(SLOTS, dtype=jnp.int32)
        spot_ids = jnp.clip(starts[:, None] + slot_ids[None, :], 0, face_count - 1)
        send_rows = jnp.where(slot_ids[None, :] < own_counts[:, None], shuffle[spot_ids], 0)
        return (by_face.reshape(4, 4, E_DEV), send_rows.astype(jnp.int32))

    def one_column(column_id):

        def per_row(row_id):
            return one_device(row_id, column_id)
        return jax.vmap(per_row)(jnp.arange(N_ROW, dtype=jnp.int32))
    fields, send_rows = jax.vmap(one_column)(column_ids)
    links = jnp.transpose(fields, (2, 3, 0, 1, 4)).reshape(4, 4, N_COL * N_ROW * E_DEV)
    return (links, send_rows.reshape(N_COL * N_ROW, N_COL, SLOTS))


def draw_neighbours(key, part):
    return build_faces(key)[0]


def draw_send_faces(key, part):
    return build_faces(key)[1]


def shard_levels(own_key, shape, pieces, low, high):
    factor_of, own = 1.0, jax.random.fold_in(own_key, 6)
    for position, shards_of in pieces:
        draws = jnp.exp(jax.random.uniform(jax.random.fold_in(own, position), (shards_of,), jnp.float32, low / len(pieces), high / len(pieces)))
        factor_of = factor_of * jnp.repeat(draws, shape[position] // shards_of).reshape([-1 if axis == position else 1 for axis in range(len(shape))])
    return factor_of


def scatter_about(rng, shape, width, limit, split=(), held_as=jnp.bfloat16):
    loudness = shard_levels(rng, shape, split, -0.22, 0.18) if split else 1.0
    values = jax.random.normal(rng, shape, jnp.float32) * width * loudness
    return jnp.minimum(jnp.maximum(values, -limit), limit).astype(held_as)


def setup_inputs(seed: int = 0) -> dict:
    splits = jax.random.split(jax.random.key(seed), 12)
    state = scatter_about(splits[0], (NQ, NB, ELEMENTS), 1.0, 6.0, ((2, 32),), jnp.float32)
    geometry = scatter_about(splits[1], (9, VQ, ELEMENTS), 1.0, 5.0, ((1, 8), (2, 4)))
    material = jnp.clip(jnp.exp(math.log(2.0) - 1.3862944 * jax.random.uniform(splits[2], (4, ELEMENTS), jnp.float32) ** shard_levels(splits[2], (4, ELEMENTS), ((1, 32),), -0.2, 0.2)), 0.5, 2.0)
    neighbours = draw_neighbours(jax.random.fold_in(splits[11], 71), 0)
    send_faces = draw_send_faces(jax.random.fold_in(splits[11], 71), 0)
    vol_eval = scatter_about(splits[5], (NB, VQ), NB ** -0.5, 1.0, (), jnp.float32)
    vol_grad = scatter_about(splits[6], (3, NB, VQ), (3 * VQ) ** -0.5, 0.3125)
    face_eval = scatter_about(splits[7], (4, NB, FQ), NB ** -0.5, 1.0, (), jnp.float32)
    face_lift = scatter_about(splits[8], (4, NB, FQ), (4 * FQ) ** -0.5, 0.625, (), jnp.float32)
    normals = scatter_about(splits[9], (3, FQ, 4, ELEMENTS), 1.0, 5.0, ((3, 32),))
    areas = jnp.clip(jnp.exp(math.log(2.0) - 1.3862944 * jax.random.uniform(splits[10], (FQ, 4, ELEMENTS), jnp.float32) ** shard_levels(splits[10], (FQ, 4, ELEMENTS), ((2, 32),), -0.2, 0.2)), 0.5, 2.0)
    return {"state": state, "geometry": geometry, "material": material, "neighbours": neighbours, "send_faces": send_faces, "vol_eval": vol_eval, "vol_grad": vol_grad, "face_eval": face_eval, "face_lift": face_lift, "normals": normals, "areas": areas}


HIGHEST = lax.Precision.HIGHEST

def normal_flux(values, lame_first, rigidity, buoyancy, normal):
    velocity = values[6:9]
    stress = values[0:6]
    normal_speed = velocity[0] * normal[0] + velocity[1] * normal[1] + velocity[2] * normal[2]
    pressure = lame_first * normal_speed
    components = [-(pressure + 2.0 * rigidity * normal[0] * velocity[0]), -(pressure + 2.0 * rigidity * normal[1] * velocity[1]), -(pressure + 2.0 * rigidity * normal[2] * velocity[2]), -rigidity * (normal[0] * velocity[1] + normal[1] * velocity[0]), -rigidity * (normal[1] * velocity[2] + normal[2] * velocity[1]), -rigidity * (normal[0] * velocity[2] + normal[2] * velocity[0]), -buoyancy * (stress[0] * normal[0] + stress[3] * normal[1] + stress[5] * normal[2]), -buoyancy * (stress[3] * normal[0] + stress[1] * normal[1] + stress[4] * normal[2]), -buoyancy * (stress[5] * normal[0] + stress[4] * normal[1] + stress[2] * normal[2])]
    return jnp.stack(components)

def volume_fluxes(points, metric, material):
    values = points.astype(jnp.float32)
    result = []
    for direction in range(3):
        normal = (metric[3 * direction], metric[3 * direction + 1], metric[3 * direction + 2])
        result.append(normal_flux(values, material[0], material[1], material[2], normal))
    return jnp.stack(result).astype(jnp.bfloat16)

def rotate_points(gathered, turning):
    full_shape = gathered.shape
    grouped = gathered.reshape(full_shape[0], full_shape[1] // 3, 3, full_shape[2], full_shape[3])
    rotated_one = jnp.roll(grouped, -1, axis=2).reshape(full_shape)
    rotated_two = jnp.roll(grouped, -2, axis=2).reshape(full_shape)
    return jnp.where(turning == 0, gathered, jnp.where(turning == 1, rotated_one, rotated_two))

def exterior(traces, gathered, face_kind, turning):
    rotated = rotate_points(gathered, turning)
    mirror = jnp.concatenate([-traces[0:6], traces[6:9]], axis=0)
    return jnp.where(face_kind == 2, mirror, jnp.where(face_kind == 3, 0.0, rotated))

def face_flux(interior, exterior_trace, interior_material, exterior_material, normals, areas):
    normal = (normals[0], normals[1], normals[2])
    interior_flux = normal_flux(interior, interior_material[0], interior_material[1], interior_material[2], normal)
    exterior_flux = normal_flux(exterior_trace, exterior_material[0], exterior_material[1], exterior_material[2], normal)
    interior_speed = jnp.sqrt((interior_material[0] + 2.0 * interior_material[1]) * interior_material[2])
    exterior_speed = jnp.sqrt((exterior_material[0] + 2.0 * exterior_material[1]) * exterior_material[2])
    penalty = 0.5 * jnp.maximum(interior_speed, exterior_speed) * areas
    return 0.5 * (interior_flux + exterior_flux) + penalty * (interior - exterior_trace)

def reference(state, geometry, material, neighbours, send_faces, vol_eval, vol_grad, face_eval, face_lift, normals, areas):
    elem_total = state.shape[2]
    traces = jnp.einsum('fbq,mbe->mqfe', face_eval, state, precision=HIGHEST)
    flat_traces = traces.reshape(9, FQ, 4 * elem_total)
    block_count = N_ROW * N_COL

    def one_block(block_id):
        start = block_id * E_DEV
        column_id = block_id // N_ROW
        row_id = block_id % N_ROW
        own_state = lax.dynamic_slice_in_dim(state, start, E_DEV, 2)
        own_geometry = lax.dynamic_slice_in_dim(geometry, start, E_DEV, 2).astype(jnp.float32)
        own_material = lax.dynamic_slice_in_dim(material, start, E_DEV, 1)
        own_links = lax.dynamic_slice_in_dim(neighbours, start, E_DEV, 2)
        own_traces = lax.dynamic_slice_in_dim(traces, start, E_DEV, 3)
        own_normals = lax.dynamic_slice_in_dim(normals, start, E_DEV, 3).astype(jnp.float32)
        own_areas = lax.dynamic_slice_in_dim(areas, start, E_DEV, 2)
        points = jnp.einsum('bq,mbe->mqe', vol_eval, own_state, precision=HIGHEST).astype(jnp.bfloat16)
        fluxes = volume_fluxes(points, own_geometry, own_material)
        volume = jnp.einsum('dbq,dmqe->mbe', vol_grad.astype(jnp.float32), fluxes.astype(jnp.float32), precision=HIGHEST)
        face_kind = own_links[0]
        peer_index = own_links[1]
        target = own_links[2]
        turning = own_links[3]
        partner_block = (peer_index * N_ROW + row_id).astype(jnp.int32)
        listed = send_faces[partner_block, column_id, jnp.minimum(target, SLOTS - 1)]
        remote_face = listed // E_DEV
        remote_elem = partner_block * E_DEV + listed % E_DEV
        local_face = target // E_DEV
        local_elem = start + target % E_DEV
        own_face = jnp.broadcast_to(jnp.arange(4, dtype=jnp.int32)[:, None], (4, E_DEV))
        own_elem = jnp.broadcast_to(start + jnp.arange(E_DEV, dtype=jnp.int32)[None, :], (4, E_DEV))
        other_face = jnp.where(face_kind == 0, local_face, jnp.where(face_kind == 1, remote_face, own_face))
        other_elem = jnp.where(face_kind == 0, local_elem, jnp.where(face_kind == 1, remote_elem, own_elem))
        global_face = (other_face * elem_total + other_elem).astype(jnp.int32)
        gathered = jnp.take(flat_traces, global_face.reshape(-1), axis=2).reshape(own_traces.shape)
        other_material = jnp.take(material[0:3], other_elem.reshape(-1).astype(jnp.int32), axis=1).reshape(3, 1, 4, E_DEV)
        exterior_trace = exterior(own_traces, gathered, face_kind, turning)
        numeric_flux = face_flux(own_traces, exterior_trace, own_material[0:3][:, None, None, :], other_material, own_normals, own_areas)
        surface = jnp.einsum('fbq,mqfe->mbe', face_lift, numeric_flux, precision=HIGHEST)
        return own_state + own_material[3][None, None, :] * (volume - surface)
    sections = lax.map(one_block, jnp.arange(block_count, dtype=jnp.int32))
    return jnp.transpose(sections, (1, 2, 0, 3)).reshape(9, NB, elem_total)
```

```python
import functools

import jax
import jax.numpy as jnp
from jax import lax
from jax.experimental import pallas as pl
from jax.experimental.pallas import tpu as pltpu
from jax.sharding import PartitionSpec as P

F32 = jnp.float32
BF16 = jnp.bfloat16
QP = 32
MESH = pl.DeviceIdType.MESH


def dot(left, right, left_dim=1, right_dim=0):
    return lax.dot_general(
        left, right, (((left_dim,), (right_dim,)), ((), ())), preferred_element_type=F32
    )


def partner(row, step, rows):
    if rows & (rows - 1):
        other = row - step
        return other + jnp.where(other < 0, rows, 0)
    total, bit = 0, 1
    while bit < rows:
        total = total + ((row // bit + step // bit) % 2) * bit
        bit *= 2
    return total


class Order:
    def __init__(self, row, rows):
        self.row, self.rows = row, rows

    def shared(self, step):
        bits = [b for b in range(1, self.rows.bit_length()) if (step >> b) & 1]
        return sum((self.row // (1 << b)) % 2 for b in bits), len(bits)

    def earlier(self, step):
        if step == 1:
            return self.row % 2 == 0
        held, count = self.shared(step)
        return held == count

    def later(self, step):
        if step == 1:
            return self.row % 2 == 1
        held, _ = self.shared(step)
        return held == 0

    def apart(self, step):
        held, count = self.shared(step)
        return (held > 0) & (held < count)


def one_hot(shape, hit):
    row_id = lax.broadcasted_iota(jnp.int32, shape, 0)
    col_id = lax.broadcasted_iota(jnp.int32, shape, 1)
    return jnp.where(hit(row_id, col_id), 1.0, 0.0).astype(BF16)


def kernel(
    rows,
    cols,
    state_in,
    geometry,
    material_in,
    neighbours_in,
    send_in,
    vol_eval_in,
    vol_grad_in,
    face_eval_in,
    face_lift_in,
    normals_in,
    areas_in,
    out,
    state,
    material,
    neighbours,
    send_faces,
    vol_eval,
    vol_grad,
    face_eval,
    face_lift,
    normals,
    areas,
    metric,
    state_low,
    traces,
    turned,
    outgoing,
    pool,
    gathered,
    points,
    fluxes,
    tests,
    normal_rows,
    area_rows,
    pick,
    far,
    load_sem,
    geo_send,
    geo_recv,
    face_send,
    face_recv,
    row_in,
    col_in,
    metric_by_row=None,
):
    row = lax.axis_index("row")
    col = lax.axis_index("col")
    quantities, basis, elems = state.shape
    local_q = geometry.shape[1]
    vol_q = vol_eval.shape[1]
    face_q = face_eval.shape[0]
    slots = send_faces.shape[2]
    direct = local_q % 16 == 0
    unit = local_q if direct else 16
    span = vol_q // 2
    tile = 3 * span + 2 * QP
    paired = rows & (rows - 1) == 0

    barrier = pltpu.get_barrier_semaphore()
    ordered = paired and rows > 1
    if ordered:
        order = Order(row, rows)
        for step in range(1, rows):

            @pl.when(order.later(step))
            def _():
                pl.semaphore_signal(
                    barrier,
                    inc=1,
                    device_id={"row": partner(row, step, rows)},
                    device_id_type=MESH,
                )

        for other in range(1, cols):

            @pl.when(col < other)
            def _():
                pl.semaphore_signal(barrier, inc=1, device_id={"col": other}, device_id_type=MESH)
    else:
        for step in range(1, rows):
            pl.semaphore_signal(
                barrier, inc=1, device_id={"row": lax.rem(row + step, rows)}, device_id_type=MESH
            )
        for step in range(1, cols):
            pl.semaphore_signal(
                barrier, inc=1, device_id={"col": lax.rem(col + step, cols)}, device_id_type=MESH
            )
    loads = {}
    pairs = [
        ("state", state_in, state),
        ("face_eval", face_eval_in, face_eval),
        ("material", material_in, material),
        ("neighbours", neighbours_in, neighbours),
        ("send_faces", send_in, send_faces),
        ("vol_eval", vol_eval_in, vol_eval),
        ("normals", normals_in, normals),
        ("areas", areas_in, areas),
        ("vol_grad", vol_grad_in, vol_grad),
        ("face_lift", face_lift_in, face_lift),
    ]
    for index, (name, source, target) in enumerate(pairs):
        loads[name] = pltpu.make_async_copy(source, target, load_sem.at[index])
        loads[name].start()
    own_copy = pltpu.make_async_copy(
        geometry.at[:, :, pl.ds(pl.multiple_of(row * elems, 128), elems)],
        metric.at[0],
        geo_recv.at[0],
    )
    own_copy.start()
    def geo_copy(step):
        peer = partner(row, step, rows) if paired else lax.rem(row + step, rows)
        return pltpu.make_async_remote_copy(
            src_ref=geometry.at[:, :, pl.ds(pl.multiple_of(peer * elems, 128), elems)],
            dst_ref=metric.at[step],
            send_sem=geo_send.at[step],
            recv_sem=geo_recv.at[step],
            device_id={"row": peer},
            device_id_type=MESH,
        )

    def face_copy(step):
        peer = lax.rem(col + step, cols)
        return pltpu.make_async_remote_copy(
            src_ref=outgoing.at[peer],
            dst_ref=pool.at[col],
            send_sem=face_send.at[step],
            recv_sem=face_recv.at[step],
            device_id={"col": peer},
            device_id_type=MESH,
        )

    geo_copies = [own_copy] + [geo_copy(step) for step in range(1, rows)]
    if ordered:
        due = col + sum(jnp.where(order.earlier(step), 1, 0) for step in range(1, rows))

        @pl.when(due > 0)
        def _():
            pl.semaphore_wait(barrier, due)

        for step in range(1, rows):

            @pl.when(order.earlier(step))
            def _():
                pl.semaphore_signal(
                    row_in.at[step],
                    inc=1,
                    device_id={"row": partner(row, step, rows)},
                    device_id_type=MESH,
                )

        for step in range(1, rows):

            @pl.when(order.earlier(step))
            def _():
                geo_copies[step].start()

        for step in range(1, cols):

            @pl.when(col >= step)
            def _():
                pl.semaphore_signal(
                    col_in.at[step], inc=1, device_id={"col": col - step}, device_id_type=MESH
                )

    else:
        pl.semaphore_wait(barrier, rows + cols - 2)
        for step in range(1, rows):
            geo_copies[step].start()

    pool[col] = jnp.zeros((slots, quantities * QP), BF16)
    loads["face_eval"].wait()

    def turning_rows(r, c):
        f = r // (3 * QP)
        turn_id = r // QP - 3 * f
        q = r % QP
        k = q % 3
        moved = k + turn_id
        moved = jnp.where(moved >= 3, moved - 3, moved)
        return (c == (q - k + moved) * 4 + f) & (q < face_q)

    turning = one_hot((12 * QP, 4 * face_q), turning_rows)
    flat = face_eval[...].reshape(4 * face_q, basis).astype(BF16)
    face_basis = dot(turning, flat).astype(BF16)
    loads["state"].wait()
    for m in range(quantities):
        state_low[m] = state[m].astype(BF16)
    loads["material"].wait()
    loads["neighbours"].wait()
    kind = neighbours[0]
    peer_index = neighbours[1]
    target = neighbours[2]
    turn = neighbours[3]
    row_ids = lax.broadcasted_iota(jnp.int32, (QP, elems), 0)
    low_rows = []
    for i in range(3):
        low_rows.append(material[i : i + 1, :].astype(BF16).astype(F32))
    for i in range(3):
        low_rows.append(material[i : i + 1, :] - low_rows[i])

    for m in range(quantities):
        found = dot(face_basis, state_low[m])
        for f in range(4):
            zero = found[3 * f * QP : (3 * f + 1) * QP]
            one = found[(3 * f + 1) * QP : (3 * f + 2) * QP]
            two = found[(3 * f + 2) * QP : (3 * f + 3) * QP]
            traces[m, f * QP : (f + 1) * QP, :] = zero
            side = turn[f : f + 1]
            chosen = jnp.where(side == 0, zero, jnp.where(side == 1, two, one))
            if m < 6:
                chosen = jnp.where(row_ids == face_q, low_rows[m], chosen)
            turned[m * QP : (m + 1) * QP, f * elems : (f + 1) * elems] = chosen.astype(BF16)

    loads["send_faces"].wait()
    same = one_hot((slots, slots), lambda r, c: r == c)
    listed = send_faces[0]
    listed_face = listed // elems
    listed_elem = listed - listed_face * elems
    face_col = dot(same, listed_face.astype(F32).astype(BF16), 1, 1)
    elem_col = dot(same, listed_elem.astype(F32).astype(BF16), 1, 1)
    listed_col = (face_col * float(elems) + elem_col).astype(jnp.int32)
    face_ids = lax.broadcasted_iota(jnp.int32, (slots, 4 * elems), 1)
    send_pick = jnp.concatenate(
        [
            jnp.where(face_ids == listed_col[:, p : p + 1], 1.0, 0.0).astype(BF16)
            for p in range(cols)
        ],
        axis=0,
    )
    listed_traces = dot(send_pick, turned[...], 1, 1).astype(BF16)
    for p in range(cols):
        outgoing[p] = listed_traces[p * slots : (p + 1) * slots]

    if ordered:
        for step in range(1, rows):

            @pl.when(order.later(step))
            def _():
                pl.semaphore_wait(row_in.at[step], 1)
                geo_copies[step].start()

        for step in range(1, rows):
            if (step // 2) & (step // 2 - 1):

                @pl.when(order.apart(step))
                def _():
                    geo_copies[step].start()
    face_copies = [face_copy(step) for step in range(1, cols)]
    for step in range(1, cols):
        if ordered:

            @pl.when(col + step >= cols)
            def _():
                face_copies[step - 1].start()
        else:
            face_copies[step - 1].start()

    loads["vol_eval"].wait()
    same_q = one_hot((vol_q, vol_q), lambda r, c: r == c)
    vol_basis = dot(same_q, vol_eval[...].astype(BF16), 1, 1).astype(BF16)
    for m in range(quantities):
        points[m] = dot(vol_basis, state_low[m])

    if ordered:
        for step in range(1, cols):

            @pl.when(col + step < cols)
            def _():
                pl.semaphore_wait(col_in.at[step], 1)
                face_copies[step - 1].start()

    elem_ids = lax.broadcasted_iota(jnp.int32, (elems, elems), 0).astype(F32).astype(BF16)
    one_low = jnp.ones((elems, elems), BF16)
    zero_low = jnp.zeros((elems, elems), BF16)
    for f in range(4):
        source = target[f : f + 1]
        near = kind[f : f + 1] == 0
        for g in range(4):
            hit = near & (source >= g * elems) & (source < (g + 1) * elems)
            wanted = jnp.where(hit, source - g * elems, -1).astype(F32).astype(BF16)
            pick[g * elems : (g + 1) * elems, :] = jnp.where(elem_ids == wanted, one_low, zero_low)
        gathered[:, f * elems : (f + 1) * elems] = dot(turned[...], pick[...])

    loads["normals"].wait()
    loads["areas"].wait()
    spread = one_hot(
        (4 * QP, 4 * face_q), lambda r, c: (c == (r % QP) * 4 + r // QP) & (r % QP < face_q)
    )
    for i in range(3):
        flat = normals[i].astype(F32).reshape(4 * face_q, elems).astype(BF16)
        normal_rows[i] = dot(spread, flat)
    flat = areas[...].reshape(4 * face_q, elems)
    high = flat.astype(BF16)
    low = (flat - high.astype(F32)).astype(BF16)
    area_rows[...] = dot(spread, high) + dot(spread, low)

    loads["vol_grad"].wait()
    loads["face_lift"].wait()

    def sent_point(h):
        def hit(k, c):
            step = h * (span // unit) + c // unit
            sender = step
            if direct:
                sender = partner(row, step, rows)
            return k == sender * unit + c % unit

        return hit

    for h in range(2):
        order = one_hot((vol_q, span), sent_point(h))
        for d in range(3):
            at = h * tile + d * span
            tests[:, at : at + span] = dot(vol_grad[d], order).astype(BF16)
    flat = face_lift[...].reshape(4 * face_q, basis).astype(BF16)
    for h in range(2):
        place = one_hot(
            (4 * face_q, 2 * QP),
            lambda r, c: (r == (c % QP) * 4 + 2 * h + c // QP) & (c % QP < face_q),
        )
        tests[:, h * tile + 3 * span : (h + 1) * tile] = (-dot(flat, place, 0, 0)).astype(BF16)

    lame = material[0:1, :]
    rigid = material[1:2, :]
    light = material[2:3, :]

    def volume_part(step, start, count, read):
        h = step // (span // unit)
        base = h * tile + (step - h * (span // unit)) * unit
        for half in range(elems // 128):
            cut = slice(half * 128, (half + 1) * 128)
            values = [points[m, pl.ds(start, count), cut] for m in range(9)]
            press = [-lame[:, cut] * values[6 + i] for i in range(3)]
            shear = [-rigid[:, cut] * values[6 + i] for i in range(3)]
            force = [-light[:, cut] * values[i] for i in range(6)]
            for d in range(3):
                n = [read(3 * d + i, cut) for i in range(3)]
                results = normal_flux(press, shear, force, n)
                at = base + d * span
                for m in range(9):
                    fluxes[m, at : at + count, cut] = results[m].astype(BF16)

    def volume_half(h):
        count = span // unit
        if direct:
            for step in range(h * count, (h + 1) * count):
                geo_copies[step].wait()
                sender = partner(row, step, rows)
                volume_part(
                    step,
                    pl.multiple_of(sender * local_q, local_q),
                    local_q,
                    lambda k, cut: metric[step, k, :, cut].astype(F32),
                )
        else:
            if h == 0:
                for step in range(rows):
                    geo_copies[step].wait()
                    metric_by_row[partner(row, step, rows)] = metric[step].astype(F32)
            group = 16 // local_q
            for block in range(h * count, (h + 1) * count):
                volume_part(
                    block,
                    block * 16,
                    16,
                    lambda k, cut: jnp.concatenate(
                        [metric_by_row[block * group + j, k, :, cut] for j in range(group)], axis=0
                    ),
                )

    pool_ids = lax.broadcasted_iota(jnp.int32, (cols * slots, elems), 0)
    for f in range(4):
        wanted = jnp.where(
            kind[f : f + 1] == 1, peer_index[f : f + 1] * slots + target[f : f + 1], -1
        )
        far[:, f * elems : (f + 1) * elems] = jnp.where(pool_ids == wanted, 1.0, 0.0).astype(BF16)
    own_speed = jnp.sqrt((lame + 2.0 * rigid) * light)

    def surface_face(f):
        lanes = slice(f * elems, (f + 1) * elems)
        free = jnp.where(kind[f : f + 1] == 2, 1.0, 0.0)
        edge = jnp.where(kind[f : f + 1] >= 2, 1.0, 0.0)
        other = []
        for i in range(3):
            high_at = i * QP + face_q
            low_at = (i + 3) * QP + face_q
            other.append(
                gathered[high_at : high_at + 1, lanes]
                + gathered[low_at : low_at + 1, lanes]
                + edge * material[i : i + 1, :]
            )
        speed = jnp.sqrt((other[0] + 2.0 * other[1]) * other[2])
        penalty_scale = 0.5 * jnp.maximum(own_speed, speed)
        for half in range(elems // 128):
            cut = slice(half * 128, (half + 1) * 128)
            a0, a1, a2 = -0.5 * lame[:, cut], -0.5 * rigid[:, cut], -0.5 * light[:, cut]
            b0, b1, b2 = -0.5 * other[0][:, cut], -0.5 * other[1][:, cut], -0.5 * other[2][:, cut]
            mirror = free[:, cut]
            for part in range(QP // 16):
                at = f * QP + part * 16
                n = [normal_rows[i, at : at + 16, cut] for i in range(3)]
                pen = penalty_scale[:, cut] * area_rows[at : at + 16, cut]
                own = [traces[m, at : at + 16, cut] for m in range(9)]
                met = []
                for m in range(9):
                    top = m * QP + part * 16
                    left = f * elems + half * 128
                    value = gathered[top : top + 16, left : left + 128]
                    part_own = mirror * own[m]
                    met.append(value - part_own if m < 6 else value + part_own)
                press = [a0 * own[6 + i] + b0 * met[6 + i] for i in range(3)]
                shear = [a1 * own[6 + i] + b1 * met[6 + i] for i in range(3)]
                force = [a2 * own[i] + b2 * met[i] for i in range(6)]
                results = normal_flux(press, shear, force, n)
                to = (f // 2) * tile + 3 * span + (f % 2) * QP + part * 16
                for m in range(9):
                    total = results[m] + pen * (own[m] - met[m])
                    fluxes[m, to : to + 16, cut] = total.astype(BF16)

    factor = material[3:4, :]
    volume_half(0)
    for copy in face_copies:
        copy.wait()
    received = pool[...].reshape(cols * slots, quantities * QP)
    gathered[...] = gathered[...] + dot(received, far[...], 0, 0)
    surface_face(0)
    surface_face(1)
    for m in range(quantities):
        out[m] = state[m] + factor * dot(tests[:, 0:tile], fluxes[m, 0:tile, :])
    surface_face(2)
    surface_face(3)
    volume_half(1)
    for m in range(quantities):
        out[m] = out[m] + factor * dot(tests[:, tile : 2 * tile], fluxes[m, tile : 2 * tile, :])


def normal_flux(press, shear, force, n):
    pressure = press[0] * n[0] + press[1] * n[1] + press[2] * n[2]
    twice = [shear[i] + shear[i] for i in range(3)]
    return [
        pressure + twice[0] * n[0],
        pressure + twice[1] * n[1],
        pressure + twice[2] * n[2],
        n[0] * shear[1] + n[1] * shear[0],
        n[1] * shear[2] + n[2] * shear[1],
        n[0] * shear[2] + n[2] * shear[0],
        force[0] * n[0] + force[3] * n[1] + force[5] * n[2],
        force[3] * n[0] + force[1] * n[1] + force[4] * n[2],
        force[5] * n[0] + force[4] * n[1] + force[2] * n[2],
    ]


def per_device(
    rows,
    cols,
    state,
    geometry,
    material,
    neighbours,
    send_faces,
    vol_eval,
    vol_grad,
    face_eval,
    face_lift,
    normals,
    areas,
):
    quantities, basis, elems = state.shape
    slots = send_faces.shape[2]
    vol_q = vol_eval.shape[1]
    local_q = geometry.shape[1]
    total = 3 * vol_q + 4 * QP
    operands = [
        state,
        geometry,
        material,
        neighbours,
        send_faces,
        vol_eval,
        vol_grad,
        jnp.transpose(face_eval, (2, 0, 1)),
        jnp.transpose(face_lift, (2, 0, 1)),
        normals,
        areas,
    ]
    staged = [pltpu.VMEM(x.shape, x.dtype) for x in operands[:1] + operands[2:]]
    scratch = staged + [
        pltpu.VMEM((rows, 9, local_q, elems), BF16),
        pltpu.VMEM((quantities, basis, elems), BF16),
        pltpu.VMEM((quantities, 4 * QP, elems), F32),
        pltpu.VMEM((quantities * QP, 4 * elems), BF16),
        pltpu.VMEM((cols, slots, quantities * QP), BF16),
        pltpu.VMEM((cols, slots, quantities * QP), BF16),
        pltpu.VMEM((quantities * QP, 4 * elems), F32),
        pltpu.VMEM((quantities, vol_q, elems), F32),
        pltpu.VMEM((quantities, total, elems), BF16),
        pltpu.VMEM((basis, total), BF16),
        pltpu.VMEM((3, 4 * QP, elems), F32),
        pltpu.VMEM((4 * QP, elems), F32),
        pltpu.VMEM((4 * elems, elems), BF16),
        pltpu.VMEM((cols * slots, 4 * elems), BF16),
        pltpu.SemaphoreType.DMA((len(staged),)),
        pltpu.SemaphoreType.DMA((rows,)),
        pltpu.SemaphoreType.DMA((rows,)),
        pltpu.SemaphoreType.DMA((cols,)),
        pltpu.SemaphoreType.DMA((cols,)),
        pltpu.SemaphoreType.REGULAR((rows,)),
        pltpu.SemaphoreType.REGULAR((cols,)),
    ]
    if local_q % 16 != 0:
        scratch.append(pltpu.VMEM((rows, 9, local_q, elems), F32))
    return pl.pallas_call(
        functools.partial(kernel, rows, cols),
        out_shape=jax.ShapeDtypeStruct(state.shape, F32),
        in_specs=[pl.BlockSpec(memory_space=pltpu.HBM)] * len(operands),
        out_specs=pl.BlockSpec(memory_space=pltpu.VMEM),
        scratch_shapes=scratch,
        compiler_params=pltpu.CompilerParams(
            collective_id=0, has_side_effects=True, vmem_limit_bytes=48 * 1024 * 1024
        ),
    )(*[pltpu.with_memory_space_constraint(x, pltpu.HBM) for x in operands])


def solution(mesh):
    return jax.shard_map(
        functools.partial(per_device, mesh.shape["row"], mesh.shape["col"]),
        mesh=mesh,
        in_specs=(
            P(None, None, ("col", "row")),
            P(None, "row", "col"),
            P(None, ("col", "row")),
            P(None, None, ("col", "row")),
            P(("col", "row"), None, None),
            P(),
            P(),
            P(),
            P(),
            P(None, None, None, ("col", "row")),
            P(None, None, ("col", "row")),
        ),
        out_specs=P(None, None, ("col", "row")),
        check_vma=False,
    )
```

```python
import functools

import jax
import jax.numpy as jnp
from jax import lax
from jax.experimental import pallas as pl
from jax.experimental.pallas import tpu as pltpu
from jax.sharding import PartitionSpec as P

F32 = jnp.float32
BF16 = jnp.bfloat16
QP = 32
MESH = pl.DeviceIdType.MESH


def dot(left, right, left_dim=1, right_dim=0):
    return lax.dot_general(
        left, right, (((left_dim,), (right_dim,)), ((), ())), preferred_element_type=F32
    )


def partner(row, step, rows):
    if rows & (rows - 1):
        other = row - step
        return other + jnp.where(other < 0, rows, 0)
    total, bit = 0, 1
    while bit < rows:
        total = total + ((row // bit + step // bit) % 2) * bit
        bit *= 2
    return total


class Order:
    def __init__(self, row, rows):
        self.row, self.rows = row, rows

    def shared(self, step):
        bits = [b for b in range(1, self.rows.bit_length()) if (step >> b) & 1]
        return sum((self.row // (1 << b)) % 2 for b in bits), len(bits)

    def earlier(self, step):
        if step == 1:
            return self.row % 2 == 0
        held, count = self.shared(step)
        return held == count

    def later(self, step):
        if step == 1:
            return self.row % 2 == 1
        held, _ = self.shared(step)
        return held == 0

    def apart(self, step):
        held, count = self.shared(step)
        return (held > 0) & (held < count)


def tiles(vol_q, unit):
    count = vol_q // unit
    groups = [list(range(count - 3)), [count - 3], [count - 2, count - 1]]
    depths = [3 * unit * len(steps) for steps in groups]
    depths[1] += 4 * QP
    flux_at = [0, depths[0], depths[0] + depths[1]]
    tests_at = [0]
    for depth in depths:
        tests_at.append(tests_at[-1] + (depth + 127) // 128 * 128)
    return groups, depths, flux_at, tests_at


def one_hot(shape, hit):
    row_id = lax.broadcasted_iota(jnp.int32, shape, 0)
    col_id = lax.broadcasted_iota(jnp.int32, shape, 1)
    return jnp.where(hit(row_id, col_id), 1.0, 0.0).astype(BF16)


def kernel(
    rows,
    cols,
    state_in,
    geometry,
    material_in,
    neighbours_in,
    send_in,
    vol_eval_in,
    vol_grad_in,
    face_eval_in,
    face_lift_in,
    normals_in,
    areas_in,
    out,
    state,
    material,
    neighbours,
    send_faces,
    vol_eval,
    vol_grad,
    face_eval,
    face_lift,
    normals,
    areas,
    metric,
    state_low,
    traces,
    turned,
    outgoing,
    pool,
    gathered,
    points,
    fluxes,
    tests,
    normal_rows,
    area_rows,
    pick,
    far,
    load_sem,
    geo_send,
    geo_recv,
    face_send,
    face_recv,
    row_in,
    col_in,
    metric_by_row=None,
):
    row = lax.axis_index("row")
    col = lax.axis_index("col")
    quantities, basis, elems = state.shape
    local_q = geometry.shape[1]
    vol_q = vol_eval.shape[1]
    face_q = face_eval.shape[0]
    slots = send_faces.shape[2]
    direct = local_q % 16 == 0
    unit = max(local_q, 16)
    groups, depths, flux_at, tests_at = tiles(vol_q, unit)
    paired = rows & (rows - 1) == 0

    barrier = pltpu.get_barrier_semaphore()
    ordered = paired and rows > 1
    if ordered:
        order = Order(row, rows)
        for step in range(1, rows):

            @pl.when(order.later(step))
            def _():
                pl.semaphore_signal(
                    barrier,
                    inc=1,
                    device_id={"row": partner(row, step, rows)},
                    device_id_type=MESH,
                )

        for other in range(1, cols):

            @pl.when(col < other)
            def _():
                pl.semaphore_signal(barrier, inc=1, device_id={"col": other}, device_id_type=MESH)
    else:
        for step in range(1, rows):
            pl.semaphore_signal(
                barrier, inc=1, device_id={"row": lax.rem(row + step, rows)}, device_id_type=MESH
            )
        for step in range(1, cols):
            pl.semaphore_signal(
                barrier, inc=1, device_id={"col": lax.rem(col + step, cols)}, device_id_type=MESH
            )
    loads = {}
    groups_of_loads = [
        [
            (face_eval_in, face_eval),
            (state_in, state),
            (material_in, material),
            (neighbours_in, neighbours),
            (send_in, send_faces),
        ],
        [
            (vol_eval_in, vol_eval),
            (normals_in, normals),
            (areas_in, areas),
            (vol_grad_in, vol_grad),
            (face_lift_in, face_lift),
        ],
    ]
    for index, group in enumerate(groups_of_loads):
        loads[index] = [
            pltpu.make_async_copy(source, target, load_sem.at[index]) for source, target in group
        ]
        for copy in loads[index]:
            copy.start()
    own_copy = pltpu.make_async_copy(
        geometry.at[:, :, pl.ds(pl.multiple_of(row * elems, 128), elems)],
        metric.at[0],
        geo_recv.at[0],
    )
    own_copy.start()
    def geo_copy(step):
        peer = partner(row, step, rows) if paired else lax.rem(row + step, rows)
        return pltpu.make_async_remote_copy(
            src_ref=geometry.at[:, :, pl.ds(pl.multiple_of(peer * elems, 128), elems)],
            dst_ref=metric.at[step],
            send_sem=geo_send,
            recv_sem=geo_recv.at[step],
            device_id={"row": peer},
            device_id_type=MESH,
        )

    def face_copy(step):
        peer = lax.rem(col + step, cols)
        return pltpu.make_async_remote_copy(
            src_ref=outgoing.at[peer],
            dst_ref=pool.at[col],
            send_sem=face_send,
            recv_sem=face_recv,
            device_id={"col": peer},
            device_id_type=MESH,
        )

    geo_copies = [own_copy] + [geo_copy(step) for step in range(1, rows)]
    if ordered:
        due = col + sum(jnp.where(order.earlier(step), 1, 0) for step in range(1, rows))

        @pl.when(due > 0)
        def _():
            pl.semaphore_wait(barrier, due)

        for step in range(1, rows):

            @pl.when(order.earlier(step))
            def _():
                pl.semaphore_signal(
                    row_in.at[step - 1],
                    inc=1,
                    device_id={"row": partner(row, step, rows)},
                    device_id_type=MESH,
                )

        for step in range(1, rows):

            @pl.when(order.earlier(step))
            def _():
                geo_copies[step].start()

        for step in range(1, cols):

            @pl.when(col >= step)
            def _():
                pl.semaphore_signal(
                    col_in.at[step - 1], inc=1, device_id={"col": col - step}, device_id_type=MESH
                )

    else:
        pl.semaphore_wait(barrier, rows + cols - 2)
        for step in range(1, rows):
            geo_copies[step].start()

    pool[col] = jnp.zeros((slots, quantities * QP), BF16)

    def turning_rows(r, c):
        f = r // (3 * QP)
        turn_id = r // QP - 3 * f
        q = r % QP
        k = q % 3
        moved = k + turn_id
        moved = jnp.where(moved >= 3, moved - 3, moved)
        return (c == (q - k + moved) * 4 + f) & (q < face_q)

    turning = one_hot((12 * QP, 4 * face_q), turning_rows)
    same = one_hot((slots, slots), lambda r, c: r == c)
    for copy in loads[0]:
        copy.wait()
    flat = face_eval[...].reshape(4 * face_q, basis).astype(BF16)
    face_basis = dot(turning, flat).astype(BF16)
    for m in range(quantities):
        state_low[m] = state[m].astype(BF16)
    kind = neighbours[0]
    peer_index = neighbours[1]
    target = neighbours[2]
    turn = neighbours[3]
    row_ids = lax.broadcasted_iota(jnp.int32, (QP, elems), 0)
    low_rows = []
    for i in range(3):
        low_rows.append(material[i : i + 1, :].astype(BF16).astype(F32))
    for i in range(3):
        low_rows.append(material[i : i + 1, :] - low_rows[i])

    for m in range(quantities):
        found = dot(face_basis, state_low[m])
        for f in range(4):
            zero = found[3 * f * QP : (3 * f + 1) * QP]
            one = found[(3 * f + 1) * QP : (3 * f + 2) * QP]
            two = found[(3 * f + 2) * QP : (3 * f + 3) * QP]
            traces[m, f * QP : (f + 1) * QP, :] = zero
            side = turn[f : f + 1]
            chosen = jnp.where(side == 0, zero, jnp.where(side == 1, two, one))
            if m < 6:
                chosen = jnp.where(row_ids == face_q, low_rows[m], chosen)
            turned[m * QP : (m + 1) * QP, f * elems : (f + 1) * elems] = chosen.astype(BF16)

    listed = send_faces[0]
    listed_face = listed // elems
    listed_elem = listed - listed_face * elems
    face_col = dot(same, listed_face.astype(F32).astype(BF16), 1, 1)
    elem_col = dot(same, listed_elem.astype(F32).astype(BF16), 1, 1)
    listed_col = (face_col * float(elems) + elem_col).astype(jnp.int32)
    face_ids = lax.broadcasted_iota(jnp.int32, (slots, 4 * elems), 1)
    send_pick = jnp.concatenate(
        [
            jnp.where(face_ids == listed_col[:, p : p + 1], 1.0, 0.0).astype(BF16)
            for p in range(cols)
        ],
        axis=0,
    )
    listed_traces = dot(send_pick, turned[...], 1, 1).astype(BF16)
    for p in range(cols):
        outgoing[p] = listed_traces[p * slots : (p + 1) * slots]

    face_copies = [face_copy(step) for step in range(1, cols)]
    for step in range(1, cols):
        if ordered:

            @pl.when(col + step >= cols)
            def _():
                face_copies[step - 1].start()
        else:
            face_copies[step - 1].start()

    if ordered:
        for step in range(1, rows):

            @pl.when(order.later(step))
            def _():
                pl.semaphore_wait(row_in.at[step - 1], 1)
                geo_copies[step].start()

        for step in range(1, rows):
            if (step // 2) & (step // 2 - 1):

                @pl.when(order.apart(step))
                def _():
                    geo_copies[step].start()

    for copy in loads[1]:
        copy.wait()
    same_q = one_hot((vol_q, vol_q), lambda r, c: r == c)
    vol_basis = dot(same_q, vol_eval[...].astype(BF16), 1, 1).astype(BF16)
    for m in range(quantities):
        points[m] = dot(vol_basis, state_low[m])

    if ordered:
        for step in range(1, cols):

            @pl.when(col + step < cols)
            def _():
                pl.semaphore_wait(col_in.at[step - 1], 1)
                face_copies[step - 1].start()

    elem_ids = lax.broadcasted_iota(jnp.int32, (elems, elems), 0).astype(F32).astype(BF16)
    one_low = jnp.ones((elems, elems), BF16)
    zero_low = jnp.zeros((elems, elems), BF16)
    for f in range(4):
        source = target[f : f + 1]
        near = kind[f : f + 1] == 0
        for g in range(4):
            hit = near & (source >= g * elems) & (source < (g + 1) * elems)
            wanted = jnp.where(hit, source - g * elems, -1).astype(F32).astype(BF16)
            pick[g * elems : (g + 1) * elems, :] = jnp.where(elem_ids == wanted, one_low, zero_low)
        gathered[:, f * elems : (f + 1) * elems] = dot(turned[...], pick[...])

    spread = one_hot(
        (4 * QP, 4 * face_q), lambda r, c: (c == (r % QP) * 4 + r // QP) & (r % QP < face_q)
    )
    for i in range(3):
        flat = normals[i].astype(F32).reshape(4 * face_q, elems).astype(BF16)
        normal_rows[i] = dot(spread, flat)
    flat = areas[...].reshape(4 * face_q, elems)
    high = flat.astype(BF16)
    low = (flat - high.astype(F32)).astype(BF16)
    area_rows[...] = dot(spread, high) + dot(spread, low)


    for t, steps in enumerate(groups):
        wide = len(steps) * unit

        def sent_point(k, c):
            step = steps[0] + c // unit
            sender = partner(row, step, rows) if direct else step
            return k == sender * unit + c % unit

        chosen_q = one_hot((vol_q, wide), sent_point)
        for d in range(3):
            at = tests_at[t] + d * wide
            tests[:, at : at + wide] = dot(vol_grad[d], chosen_q).astype(BF16)
    flat = face_lift[...].reshape(4 * face_q, basis).astype(BF16)
    place = one_hot(
        (4 * face_q, 4 * QP),
        lambda r, c: (r == (c % QP) * 4 + c // QP) & (c % QP < face_q),
    )
    at = tests_at[1] + 3 * unit * len(groups[1])
    tests[:, at : at + 4 * QP] = (-dot(flat, place, 0, 0)).astype(BF16)

    lame = material[0:1, :]
    rigid = material[1:2, :]
    light = material[2:3, :]

    def volume_part(step, start, count, read):
        t = [step in steps for steps in groups].index(True)
        wide = len(groups[t]) * unit
        base = flux_at[t] + (step - groups[t][0]) * unit
        for half in range(elems // 128):
            cut = slice(half * 128, (half + 1) * 128)
            values = [points[m, pl.ds(start, count), cut] for m in range(9)]
            press = [-lame[:, cut] * values[6 + i] for i in range(3)]
            shear = [-rigid[:, cut] * values[6 + i] for i in range(3)]
            force = [-light[:, cut] * values[i] for i in range(6)]
            for d in range(3):
                n = [read(3 * d + i, cut) for i in range(3)]
                results = normal_flux(press, shear, force, n)
                at = base + d * wide
                for m in range(9):
                    fluxes[m, at : at + count, cut] = results[m].astype(BF16)

    def arrived(step):
        if step == 0:
            own_copy.wait()
        else:
            geo_copies[step].wait_recv()

    def volume(steps):
        if direct:
            for step in steps:
                arrived(step)
                sender = partner(row, step, rows)
                volume_part(
                    step,
                    pl.multiple_of(sender * local_q, local_q),
                    local_q,
                    lambda k, cut: metric[step, k, :, cut].astype(F32),
                )
        else:
            if steps[0] == 0:
                for step in range(rows):
                    arrived(step)
                    metric_by_row[partner(row, step, rows)] = metric[step].astype(F32)
            group = 16 // local_q
            for block in steps:
                volume_part(
                    block,
                    block * 16,
                    16,
                    lambda k, cut: jnp.concatenate(
                        [metric_by_row[block * group + j, k, :, cut] for j in range(group)], axis=0
                    ),
                )

    def contract(t, m):
        left = tests[:, tests_at[t] : tests_at[t] + depths[t]]
        return dot(left, fluxes[m, flux_at[t] : flux_at[t] + depths[t], :])

    pool_ids = lax.broadcasted_iota(jnp.int32, (cols * slots, elems), 0)
    for f in range(4):
        wanted = jnp.where(
            kind[f : f + 1] == 1, peer_index[f : f + 1] * slots + target[f : f + 1], -1
        )
        far[:, f * elems : (f + 1) * elems] = jnp.where(pool_ids == wanted, 1.0, 0.0).astype(BF16)
    own_speed = jnp.sqrt((lame + 2.0 * rigid) * light)

    def surface_face(f):
        lanes = slice(f * elems, (f + 1) * elems)
        free = jnp.where(kind[f : f + 1] == 2, 1.0, 0.0)
        edge = jnp.where(kind[f : f + 1] >= 2, 1.0, 0.0)
        other = []
        for i in range(3):
            high_at = i * QP + face_q
            low_at = (i + 3) * QP + face_q
            other.append(
                gathered[high_at : high_at + 1, lanes]
                + gathered[low_at : low_at + 1, lanes]
                + edge * material[i : i + 1, :]
            )
        speed = jnp.sqrt((other[0] + 2.0 * other[1]) * other[2])
        penalty_scale = 0.5 * jnp.maximum(own_speed, speed)
        for half in range(elems // 128):
            cut = slice(half * 128, (half + 1) * 128)
            a0, a1, a2 = -0.5 * lame[:, cut], -0.5 * rigid[:, cut], -0.5 * light[:, cut]
            b0, b1, b2 = -0.5 * other[0][:, cut], -0.5 * other[1][:, cut], -0.5 * other[2][:, cut]
            mirror = free[:, cut]
            for part in range(QP // 16):
                at = f * QP + part * 16
                n = [normal_rows[i, at : at + 16, cut] for i in range(3)]
                pen = penalty_scale[:, cut] * area_rows[at : at + 16, cut]
                own = [traces[m, at : at + 16, cut] for m in range(9)]
                met = []
                for m in range(9):
                    top = m * QP + part * 16
                    left = f * elems + half * 128
                    value = gathered[top : top + 16, left : left + 128]
                    part_own = mirror * own[m]
                    met.append(value - part_own if m < 6 else value + part_own)
                press = [a0 * own[6 + i] + b0 * met[6 + i] for i in range(3)]
                shear = [a1 * own[6 + i] + b1 * met[6 + i] for i in range(3)]
                force = [a2 * own[i] + b2 * met[i] for i in range(6)]
                results = normal_flux(press, shear, force, n)
                to = flux_at[1] + 3 * unit * len(groups[1]) + f * QP + part * 16
                for m in range(9):
                    total = results[m] + pen * (own[m] - met[m])
                    fluxes[m, to : to + 16, cut] = total.astype(BF16)

    factor = material[3:4, :]
    volume(groups[0])
    for m in range(quantities):
        out[m] = contract(0, m)
    volume(groups[1])
    whole = pool.at[pl.ds(0, cols - 1)]
    pltpu.make_async_copy(whole, whole, face_recv).wait()
    received = pool[...].reshape(cols * slots, quantities * QP)
    gathered[...] = gathered[...] + dot(received, far[...], 0, 0)
    for f in range(4):
        surface_face(f)
    for m in range(quantities):
        out[m] = out[m] + contract(1, m)
    volume(groups[2])
    whole = metric.at[pl.ds(0, rows - 1)]
    pltpu.make_async_copy(whole, whole, geo_send).wait()
    whole = outgoing.at[pl.ds(0, cols - 1)]
    pltpu.make_async_copy(whole, whole, face_send).wait()
    for m in range(quantities):
        out[m] = state[m] + factor * (out[m] + contract(2, m))


def normal_flux(press, shear, force, n):
    pressure = press[0] * n[0] + press[1] * n[1] + press[2] * n[2]
    twice = [shear[i] + shear[i] for i in range(3)]
    return [
        pressure + twice[0] * n[0],
        pressure + twice[1] * n[1],
        pressure + twice[2] * n[2],
        n[0] * shear[1] + n[1] * shear[0],
        n[1] * shear[2] + n[2] * shear[1],
        n[0] * shear[2] + n[2] * shear[0],
        force[0] * n[0] + force[3] * n[1] + force[5] * n[2],
        force[3] * n[0] + force[1] * n[1] + force[4] * n[2],
        force[5] * n[0] + force[4] * n[1] + force[2] * n[2],
    ]


def per_device(
    rows,
    cols,
    state,
    geometry,
    material,
    neighbours,
    send_faces,
    vol_eval,
    vol_grad,
    face_eval,
    face_lift,
    normals,
    areas,
):
    quantities, basis, elems = state.shape
    slots = send_faces.shape[2]
    vol_q = vol_eval.shape[1]
    local_q = geometry.shape[1]
    total = 3 * vol_q + 4 * QP
    tests_at = tiles(vol_q, max(local_q, 16))[3]
    operands = [
        state,
        geometry,
        material,
        neighbours,
        send_faces,
        vol_eval,
        vol_grad,
        jnp.transpose(face_eval, (2, 0, 1)),
        jnp.transpose(face_lift, (2, 0, 1)),
        normals,
        areas,
    ]
    staged = [pltpu.VMEM(x.shape, x.dtype) for x in operands[:1] + operands[2:]]
    scratch = staged + [
        pltpu.VMEM((rows, 9, local_q, elems), BF16),
        pltpu.VMEM((quantities, basis, elems), BF16),
        pltpu.VMEM((quantities, 4 * QP, elems), F32),
        pltpu.VMEM((quantities * QP, 4 * elems), BF16),
        pltpu.VMEM((cols, slots, quantities * QP), BF16),
        pltpu.VMEM((cols, slots, quantities * QP), BF16),
        pltpu.VMEM((quantities * QP, 4 * elems), F32),
        pltpu.VMEM((quantities, vol_q, elems), F32),
        pltpu.VMEM((quantities, total, elems), BF16),
        pltpu.VMEM((basis, tests_at[-1]), BF16),
        pltpu.VMEM((3, 4 * QP, elems), F32),
        pltpu.VMEM((4 * QP, elems), F32),
        pltpu.VMEM((4 * elems, elems), BF16),
        pltpu.VMEM((cols * slots, 4 * elems), BF16),
        pltpu.SemaphoreType.DMA((2,)),
        pltpu.SemaphoreType.DMA,
        pltpu.SemaphoreType.DMA((rows,)),
        pltpu.SemaphoreType.DMA,
        pltpu.SemaphoreType.DMA,
        pltpu.SemaphoreType.REGULAR((rows - 1,)),
        pltpu.SemaphoreType.REGULAR((cols - 1,)),
    ]
    if local_q % 16 != 0:
        scratch.append(pltpu.VMEM((rows, 9, local_q, elems), F32))
    return pl.pallas_call(
        functools.partial(kernel, rows, cols),
        out_shape=jax.ShapeDtypeStruct(state.shape, F32),
        in_specs=[pl.BlockSpec(memory_space=pltpu.HBM)] * len(operands),
        out_specs=pl.BlockSpec(memory_space=pltpu.VMEM),
        scratch_shapes=scratch,
        compiler_params=pltpu.CompilerParams(
            collective_id=0, has_side_effects=True, vmem_limit_bytes=48 * 1024 * 1024
        ),
    )(*[pltpu.with_memory_space_constraint(x, pltpu.HBM) for x in operands])


def solution(mesh):
    return jax.shard_map(
        functools.partial(per_device, mesh.shape["row"], mesh.shape["col"]),
        mesh=mesh,
        in_specs=(
            P(None, None, ("col", "row")),
            P(None, "row", "col"),
            P(None, ("col", "row")),
            P(None, None, ("col", "row")),
            P(("col", "row"), None, None),
            P(),
            P(),
            P(),
            P(),
            P(None, None, None, ("col", "row")),
            P(None, None, ("col", "row")),
        ),
        out_specs=P(None, None, ("col", "row")),
        check_vma=False,
    )
```

```python
import functools

import jax
import jax.numpy as jnp
from jax import lax
from jax.experimental import pallas as pl
from jax.experimental.pallas import tpu as pltpu
from jax.sharding import PartitionSpec as P

F32 = jnp.float32
BF16 = jnp.bfloat16
QP = 32
MESH = pl.DeviceIdType.MESH


def dot(left, right, left_dim=1, right_dim=0):
    return lax.dot_general(
        left, right, (((left_dim,), (right_dim,)), ((), ())), preferred_element_type=F32
    )


def partner(row, step, rows):
    if rows & (rows - 1):
        other = row - step
        return other + jnp.where(other < 0, rows, 0)
    total, bit = 0, 1
    while bit < rows:
        total = total + ((row // bit + step // bit) % 2) * bit
        bit *= 2
    return total


class Order:
    def __init__(self, row, rows):
        self.row, self.rows = row, rows

    def shared(self, step):
        bits = [b for b in range(1, self.rows.bit_length()) if (step >> b) & 1]
        return sum((self.row // (1 << b)) % 2 for b in bits), len(bits)

    def earlier(self, step):
        if step == 1:
            return self.row % 2 == 0
        held, count = self.shared(step)
        return held == count

    def later(self, step):
        if step == 1:
            return self.row % 2 == 1
        held, _ = self.shared(step)
        return held == 0

    def apart(self, step):
        held, count = self.shared(step)
        return (held > 0) & (held < count)


def tiles(vol_q, unit):
    count = vol_q // unit
    groups = [list(range(count - 3)), [count - 3, count - 2, count - 1]]
    depths = [3 * unit * len(steps) for steps in groups] + [4 * QP]
    flux_at = [0, depths[0], depths[0] + depths[1]]
    tests_at = [0]
    for depth in depths:
        tests_at.append(tests_at[-1] + (depth + 127) // 128 * 128)
    return groups, depths, flux_at, tests_at


def one_hot(shape, hit):
    row_id = lax.broadcasted_iota(jnp.int32, shape, 0)
    col_id = lax.broadcasted_iota(jnp.int32, shape, 1)
    return jnp.where(hit(row_id, col_id), 1.0, 0.0).astype(BF16)


def kernel(
    rows,
    cols,
    state_in,
    geometry,
    material_in,
    neighbours_in,
    send_in,
    vol_eval_in,
    vol_grad_in,
    face_eval_in,
    face_lift_in,
    normals_in,
    areas_in,
    out,
    state,
    material,
    neighbours,
    send_faces,
    vol_eval,
    vol_grad,
    face_eval,
    face_lift,
    normals,
    areas,
    metric,
    state_low,
    traces,
    turned,
    outgoing,
    pool,
    gathered,
    points,
    fluxes,
    tests,
    normal_rows,
    area_rows,
    pick,
    far,
    load_sem,
    geo_send,
    geo_recv,
    face_send,
    face_recv,
    row_in,
    col_in,
    metric_by_row=None,
):
    row = lax.axis_index("row")
    col = lax.axis_index("col")
    quantities, basis, elems = state.shape
    local_q = geometry.shape[1]
    vol_q = vol_eval.shape[1]
    face_q = face_eval.shape[0]
    slots = send_faces.shape[2]
    direct = local_q % 16 == 0
    unit = max(local_q, 16)
    groups, depths, flux_at, tests_at = tiles(vol_q, unit)
    paired = rows & (rows - 1) == 0

    barrier = pltpu.get_barrier_semaphore()
    ordered = paired and rows > 1
    if ordered:
        order = Order(row, rows)
        for step in range(1, rows):

            @pl.when(order.later(step))
            def _():
                pl.semaphore_signal(
                    barrier,
                    inc=1,
                    device_id={"row": partner(row, step, rows)},
                    device_id_type=MESH,
                )

        for other in range(1, cols):

            @pl.when(col < other)
            def _():
                pl.semaphore_signal(barrier, inc=1, device_id={"col": other}, device_id_type=MESH)
    else:
        for step in range(1, rows):
            pl.semaphore_signal(
                barrier, inc=1, device_id={"row": lax.rem(row + step, rows)}, device_id_type=MESH
            )
        for step in range(1, cols):
            pl.semaphore_signal(
                barrier, inc=1, device_id={"col": lax.rem(col + step, cols)}, device_id_type=MESH
            )
    loads = {}
    groups_of_loads = [
        [
            (face_eval_in, face_eval),
            (state_in, state),
            (material_in, material),
            (neighbours_in, neighbours),
            (send_in, send_faces),
        ],
        [
            (vol_eval_in, vol_eval),
            (normals_in, normals),
            (areas_in, areas),
            (vol_grad_in, vol_grad),
            (face_lift_in, face_lift),
        ],
    ]
    for index, group in enumerate(groups_of_loads):
        loads[index] = [
            pltpu.make_async_copy(source, target, load_sem.at[index]) for source, target in group
        ]
        for copy in loads[index]:
            copy.start()
    own_copy = pltpu.make_async_copy(
        geometry.at[:, :, pl.ds(pl.multiple_of(row * elems, 128), elems)],
        metric.at[0],
        geo_recv.at[0],
    )
    own_copy.start()
    def geo_copy(step):
        peer = partner(row, step, rows) if paired else lax.rem(row + step, rows)
        return pltpu.make_async_remote_copy(
            src_ref=geometry.at[:, :, pl.ds(pl.multiple_of(peer * elems, 128), elems)],
            dst_ref=metric.at[step],
            send_sem=geo_send,
            recv_sem=geo_recv.at[step],
            device_id={"row": peer},
            device_id_type=MESH,
        )

    def face_copy(step):
        peer = lax.rem(col + step, cols)
        return pltpu.make_async_remote_copy(
            src_ref=outgoing.at[peer],
            dst_ref=pool.at[col],
            send_sem=face_send,
            recv_sem=face_recv,
            device_id={"col": peer},
            device_id_type=MESH,
        )

    def later_sends(steps, where=True):
        for step in steps:

            @pl.when(order.later(step) & where)
            def _():
                pl.semaphore_wait(row_in.at[step - 1], 1)
                geo_copies[step].start()

    geo_copies = [own_copy] + [geo_copy(step) for step in range(1, rows)]
    if ordered:
        due = col + sum(jnp.where(order.earlier(step), 1, 0) for step in range(1, rows))

        @pl.when(due > 0)
        def _():
            pl.semaphore_wait(barrier, due)

        for step in range(1, rows):

            @pl.when(order.earlier(step))
            def _():
                pl.semaphore_signal(
                    row_in.at[step - 1],
                    inc=1,
                    device_id={"row": partner(row, step, rows)},
                    device_id_type=MESH,
                )

        for step in range(1, rows):

            @pl.when(order.earlier(step))
            def _():
                geo_copies[step].start()

        for step in range(1, cols):

            @pl.when(col >= step)
            def _():
                pl.semaphore_signal(
                    col_in.at[step - 1], inc=1, device_id={"col": col - step}, device_id_type=MESH
                )

    else:
        pl.semaphore_wait(barrier, rows + cols - 2)
        for step in range(1, rows):
            geo_copies[step].start()

    wire = pool.shape[2]
    pool[col] = jnp.zeros((slots, wire), BF16)

    def turning_rows(r, c):
        f = r // (3 * QP)
        turn_id = r // QP - 3 * f
        q = r % QP
        k = q % 3
        moved = k + turn_id
        moved = jnp.where(moved >= 3, moved - 3, moved)
        return (c == (q - k + moved) * 4 + f) & (q < face_q)

    turning = one_hot((12 * QP, 4 * face_q), turning_rows)
    same = one_hot((slots, slots), lambda r, c: r == c)
    narrow = one_hot(
        (quantities * QP, wire),
        lambda r, c: (c == (r // QP) * (face_q + 1) + r % QP) & (r % QP <= face_q),
    )
    for copy in loads[0]:
        copy.wait()
    flat = face_eval[...].reshape(4 * face_q, basis).astype(BF16)
    face_basis = dot(turning, flat).astype(BF16)
    for m in range(quantities):
        state_low[m] = state[m].astype(BF16)
    kind = neighbours[0]
    peer_index = neighbours[1]
    target = neighbours[2]
    turn = neighbours[3]
    row_ids = lax.broadcasted_iota(jnp.int32, (QP, elems), 0)
    low_rows = []
    for i in range(3):
        low_rows.append(material[i : i + 1, :].astype(BF16).astype(F32))
    for i in range(3):
        low_rows.append(material[i : i + 1, :] - low_rows[i])

    for m in range(quantities):
        found = dot(face_basis, state_low[m])
        for f in range(4):
            zero = found[3 * f * QP : (3 * f + 1) * QP]
            one = found[(3 * f + 1) * QP : (3 * f + 2) * QP]
            two = found[(3 * f + 2) * QP : (3 * f + 3) * QP]
            traces[m, f * QP : (f + 1) * QP, :] = zero
            side = turn[f : f + 1]
            chosen = jnp.where(side == 0, zero, jnp.where(side == 1, two, one))
            if m < 6:
                chosen = jnp.where(row_ids == face_q, low_rows[m], chosen)
            turned[m * QP : (m + 1) * QP, f * elems : (f + 1) * elems] = chosen.astype(BF16)

    if ordered:
        later_sends(range(1, rows - 2))
        later_sends(range(rows - 2, rows), row >= 2)
        for step in range(1, rows):
            if (step // 2) & (step // 2 - 1):

                @pl.when(order.apart(step))
                def _():
                    geo_copies[step].start()

    listed = send_faces[0]
    listed_face = listed // elems
    listed_elem = listed - listed_face * elems
    face_col = dot(same, listed_face.astype(F32).astype(BF16), 1, 1)
    elem_col = dot(same, listed_elem.astype(F32).astype(BF16), 1, 1)
    listed_col = (face_col * float(elems) + elem_col).astype(jnp.int32)
    face_ids = lax.broadcasted_iota(jnp.int32, (slots, 4 * elems), 1)
    send_pick = jnp.concatenate(
        [
            jnp.where(face_ids == listed_col[:, p : p + 1], 1.0, 0.0).astype(BF16)
            for p in range(cols)
        ],
        axis=0,
    )
    listed_traces = dot(send_pick, turned[...], 1, 1).astype(BF16)
    listed_traces = dot(listed_traces, narrow).astype(BF16)
    for p in range(cols):
        outgoing[p] = listed_traces[p * slots : (p + 1) * slots]

    face_copies = [face_copy(step) for step in range(1, cols)]
    for step in range(1, cols):
        if ordered:

            @pl.when(col + step >= cols)
            def _():
                face_copies[step - 1].start()
        else:
            face_copies[step - 1].start()

    if ordered:
        later_sends(range(rows - 2, rows), row < 2)

    for copy in loads[1]:
        copy.wait()
    same_q = one_hot((vol_q, vol_q), lambda r, c: r == c)
    vol_basis = dot(same_q, vol_eval[...].astype(BF16), 1, 1).astype(BF16)
    for m in range(quantities):
        points[m] = dot(vol_basis, state_low[m])

    if ordered:
        for step in range(1, cols):

            @pl.when(col + step < cols)
            def _():
                pl.semaphore_wait(col_in.at[step - 1], 1)
                face_copies[step - 1].start()

    elem_ids = lax.broadcasted_iota(jnp.int32, (elems, elems), 0).astype(F32).astype(BF16)
    one_low = jnp.ones((elems, elems), BF16)
    zero_low = jnp.zeros((elems, elems), BF16)
    for f in range(4):
        source = target[f : f + 1]
        near = kind[f : f + 1] == 0
        for g in range(4):
            hit = near & (source >= g * elems) & (source < (g + 1) * elems)
            wanted = jnp.where(hit, source - g * elems, -1).astype(F32).astype(BF16)
            pick[g * elems : (g + 1) * elems, :] = jnp.where(elem_ids == wanted, one_low, zero_low)
        gathered[:, f * elems : (f + 1) * elems] = dot(turned[...], pick[...])

    spread = one_hot(
        (4 * QP, 4 * face_q), lambda r, c: (c == (r % QP) * 4 + r // QP) & (r % QP < face_q)
    )
    for i in range(3):
        flat = normals[i].astype(F32).reshape(4 * face_q, elems).astype(BF16)
        normal_rows[i] = dot(spread, flat)
    flat = areas[...].reshape(4 * face_q, elems)
    high = flat.astype(BF16)
    low = (flat - high.astype(F32)).astype(BF16)
    area_rows[...] = dot(spread, high) + dot(spread, low)


    for t, steps in enumerate(groups):
        wide = len(steps) * unit

        def sent_point(k, c):
            step = steps[0] + c // unit
            sender = partner(row, step, rows) if direct else step
            return k == sender * unit + c % unit

        chosen_q = one_hot((vol_q, wide), sent_point)
        for d in range(3):
            at = tests_at[t] + d * wide
            tests[:, at : at + wide] = dot(vol_grad[d], chosen_q).astype(BF16)
    flat = face_lift[...].reshape(4 * face_q, basis).astype(BF16)
    place = one_hot(
        (4 * face_q, 4 * QP),
        lambda r, c: (r == (c % QP) * 4 + c // QP) & (c % QP < face_q),
    )
    at = tests_at[2]
    tests[:, at : at + 4 * QP] = (-dot(flat, place, 0, 0)).astype(BF16)

    lame = material[0:1, :]
    rigid = material[1:2, :]
    light = material[2:3, :]

    def volume_part(step, start, count, read):
        t = [step in steps for steps in groups].index(True)
        wide = len(groups[t]) * unit
        base = flux_at[t] + (step - groups[t][0]) * unit
        for half in range(elems // 128):
            cut = slice(half * 128, (half + 1) * 128)
            values = [points[m, pl.ds(start, count), cut] for m in range(9)]
            press = [-lame[:, cut] * values[6 + i] for i in range(3)]
            shear = [-rigid[:, cut] * values[6 + i] for i in range(3)]
            force = [-light[:, cut] * values[i] for i in range(6)]
            for d in range(3):
                n = [read(3 * d + i, cut) for i in range(3)]
                results = normal_flux(press, shear, force, n)
                at = base + d * wide
                for m in range(9):
                    fluxes[m, at : at + count, cut] = results[m].astype(BF16)

    def arrived(step):
        if step == 0:
            own_copy.wait()
        else:
            geo_copies[step].wait_recv()

    def volume(steps):
        if direct:
            for step in steps:
                arrived(step)
                sender = partner(row, step, rows)
                volume_part(
                    step,
                    pl.multiple_of(sender * local_q, local_q),
                    local_q,
                    lambda k, cut: metric[step, k, :, cut].astype(F32),
                )
        else:
            if steps[0] == 0:
                for step in range(rows):
                    arrived(step)
                    metric_by_row[partner(row, step, rows)] = metric[step].astype(F32)
            group = 16 // local_q
            for block in steps:
                volume_part(
                    block,
                    block * 16,
                    16,
                    lambda k, cut: jnp.concatenate(
                        [metric_by_row[block * group + j, k, :, cut] for j in range(group)], axis=0
                    ),
                )

    def contract(t, m):
        left = tests[:, tests_at[t] : tests_at[t] + depths[t]]
        return dot(left, fluxes[m, flux_at[t] : flux_at[t] + depths[t], :])

    pool_ids = lax.broadcasted_iota(jnp.int32, (cols * slots, elems), 0)
    for f in range(4):
        wanted = jnp.where(
            kind[f : f + 1] == 1, peer_index[f : f + 1] * slots + target[f : f + 1], -1
        )
        far[:, f * elems : (f + 1) * elems] = jnp.where(pool_ids == wanted, 1.0, 0.0).astype(BF16)
    own_speed = jnp.sqrt((lame + 2.0 * rigid) * light)

    def surface_face(f):
        lanes = slice(f * elems, (f + 1) * elems)
        free = jnp.where(kind[f : f + 1] == 2, 1.0, 0.0)
        edge = jnp.where(kind[f : f + 1] >= 2, 1.0, 0.0)
        other = []
        for i in range(3):
            high_at = i * QP + face_q
            low_at = (i + 3) * QP + face_q
            other.append(
                gathered[high_at : high_at + 1, lanes]
                + gathered[low_at : low_at + 1, lanes]
                + edge * material[i : i + 1, :]
            )
        speed = jnp.sqrt((other[0] + 2.0 * other[1]) * other[2])
        penalty_scale = 0.5 * jnp.maximum(own_speed, speed)
        for half in range(elems // 128):
            cut = slice(half * 128, (half + 1) * 128)
            a0, a1, a2 = -0.5 * lame[:, cut], -0.5 * rigid[:, cut], -0.5 * light[:, cut]
            b0, b1, b2 = -0.5 * other[0][:, cut], -0.5 * other[1][:, cut], -0.5 * other[2][:, cut]
            mirror = free[:, cut]
            for part in range(QP // 16):
                at = f * QP + part * 16
                n = [normal_rows[i, at : at + 16, cut] for i in range(3)]
                pen = penalty_scale[:, cut] * area_rows[at : at + 16, cut]
                own = [traces[m, at : at + 16, cut] for m in range(9)]
                met = []
                for m in range(9):
                    top = m * QP + part * 16
                    left = f * elems + half * 128
                    value = gathered[top : top + 16, left : left + 128]
                    part_own = mirror * own[m]
                    met.append(value - part_own if m < 6 else value + part_own)
                press = [a0 * own[6 + i] + b0 * met[6 + i] for i in range(3)]
                shear = [a1 * own[6 + i] + b1 * met[6 + i] for i in range(3)]
                force = [a2 * own[i] + b2 * met[i] for i in range(6)]
                results = normal_flux(press, shear, force, n)
                to = flux_at[2] + f * QP + part * 16
                for m in range(9):
                    total = results[m] + pen * (own[m] - met[m])
                    fluxes[m, to : to + 16, cut] = total.astype(BF16)

    factor = material[3:4, :]
    volume(groups[0])
    for m in range(quantities):
        out[m] = contract(0, m)
    whole = pool.at[pl.ds(0, cols - 1)]
    pltpu.make_async_copy(whole, whole, face_recv).wait()
    received = pool[...].reshape(cols * slots, wire)
    received = dot(narrow, received, 1, 1).astype(BF16)
    gathered[...] = gathered[...] + dot(received, far[...])
    for f in range(4):
        surface_face(f)
    for m in range(quantities):
        out[m] = out[m] + contract(2, m)
    volume(groups[1])
    whole = metric.at[pl.ds(0, rows - 1)]
    pltpu.make_async_copy(whole, whole, geo_send).wait()
    whole = outgoing.at[pl.ds(0, cols - 1)]
    pltpu.make_async_copy(whole, whole, face_send).wait()
    for m in range(quantities):
        out[m] = state[m] + factor * (out[m] + contract(1, m))


def normal_flux(press, shear, force, n):
    pressure = press[0] * n[0] + press[1] * n[1] + press[2] * n[2]
    twice = [shear[i] + shear[i] for i in range(3)]
    return [
        pressure + twice[0] * n[0],
        pressure + twice[1] * n[1],
        pressure + twice[2] * n[2],
        n[0] * shear[1] + n[1] * shear[0],
        n[1] * shear[2] + n[2] * shear[1],
        n[0] * shear[2] + n[2] * shear[0],
        force[0] * n[0] + force[3] * n[1] + force[5] * n[2],
        force[3] * n[0] + force[1] * n[1] + force[4] * n[2],
        force[5] * n[0] + force[4] * n[1] + force[2] * n[2],
    ]


def per_device(
    rows,
    cols,
    state,
    geometry,
    material,
    neighbours,
    send_faces,
    vol_eval,
    vol_grad,
    face_eval,
    face_lift,
    normals,
    areas,
):
    quantities, basis, elems = state.shape
    slots = send_faces.shape[2]
    vol_q = vol_eval.shape[1]
    local_q = geometry.shape[1]
    total = 3 * vol_q + 4 * QP
    wire = (quantities * (face_eval.shape[2] + 1) + 127) // 128 * 128
    tests_at = tiles(vol_q, max(local_q, 16))[3]
    operands = [
        state,
        geometry,
        material,
        neighbours,
        send_faces,
        vol_eval,
        vol_grad,
        jnp.transpose(face_eval, (2, 0, 1)),
        jnp.transpose(face_lift, (2, 0, 1)),
        normals,
        areas,
    ]
    staged = [pltpu.VMEM(x.shape, x.dtype) for x in operands[:1] + operands[2:]]
    scratch = staged + [
        pltpu.VMEM((rows, 9, local_q, elems), BF16),
        pltpu.VMEM((quantities, basis, elems), BF16),
        pltpu.VMEM((quantities, 4 * QP, elems), F32),
        pltpu.VMEM((quantities * QP, 4 * elems), BF16),
        pltpu.VMEM((cols, slots, wire), BF16),
        pltpu.VMEM((cols, slots, wire), BF16),
        pltpu.VMEM((quantities * QP, 4 * elems), F32),
        pltpu.VMEM((quantities, vol_q, elems), F32),
        pltpu.VMEM((quantities, total, elems), BF16),
        pltpu.VMEM((basis, tests_at[-1]), BF16),
        pltpu.VMEM((3, 4 * QP, elems), F32),
        pltpu.VMEM((4 * QP, elems), F32),
        pltpu.VMEM((4 * elems, elems), BF16),
        pltpu.VMEM((cols * slots, 4 * elems), BF16),
        pltpu.SemaphoreType.DMA((2,)),
        pltpu.SemaphoreType.DMA,
        pltpu.SemaphoreType.DMA((rows,)),
        pltpu.SemaphoreType.DMA,
        pltpu.SemaphoreType.DMA,
        pltpu.SemaphoreType.REGULAR((rows - 1,)),
        pltpu.SemaphoreType.REGULAR((cols - 1,)),
    ]
    if local_q % 16 != 0:
        scratch.append(pltpu.VMEM((rows, 9, local_q, elems), F32))
    return pl.pallas_call(
        functools.partial(kernel, rows, cols),
        out_shape=jax.ShapeDtypeStruct(state.shape, F32),
        in_specs=[pl.BlockSpec(memory_space=pltpu.HBM)] * len(operands),
        out_specs=pl.BlockSpec(memory_space=pltpu.VMEM),
        scratch_shapes=scratch,
        compiler_params=pltpu.CompilerParams(
            collective_id=0, has_side_effects=True, vmem_limit_bytes=48 * 1024 * 1024
        ),
    )(*[pltpu.with_memory_space_constraint(x, pltpu.HBM) for x in operands])


def solution(mesh):
    return jax.shard_map(
        functools.partial(per_device, mesh.shape["row"], mesh.shape["col"]),
        mesh=mesh,
        in_specs=(
            P(None, None, ("col", "row")),
            P(None, "row", "col"),
            P(None, ("col", "row")),
            P(None, None, ("col", "row")),
            P(("col", "row"), None, None),
            P(),
            P(),
            P(),
            P(),
            P(None, None, None, ("col", "row")),
            P(None, None, ("col", "row")),
        ),
        out_specs=P(None, None, ("col", "row")),
        check_vma=False,
    )
```

```python
import functools

import jax
import jax.numpy as jnp
from jax import lax
from jax.experimental import pallas as pl
from jax.experimental.pallas import tpu as pltpu
from jax.sharding import PartitionSpec as P

F32 = jnp.float32
BF16 = jnp.bfloat16
QP = 32
MESH = pl.DeviceIdType.MESH


def dot(left, right, left_dim=1, right_dim=0):
    return lax.dot_general(
        left, right, (((left_dim,), (right_dim,)), ((), ())), preferred_element_type=F32
    )


def partner(row, step, rows):
    if rows & (rows - 1):
        other = row - step
        return other + jnp.where(other < 0, rows, 0)
    total, bit = 0, 1
    while bit < rows:
        total = total + ((row // bit + step // bit) % 2) * bit
        bit *= 2
    return total


class Order:
    def __init__(self, row, rows):
        self.row, self.rows = row, rows

    def shared(self, step):
        bits = [b for b in range(1, self.rows.bit_length()) if (step >> b) & 1]
        return sum((self.row // (1 << b)) % 2 for b in bits), len(bits)

    def earlier(self, step):
        if step == 1:
            return self.row % 2 == 0
        held, count = self.shared(step)
        return held == count

    def later(self, step):
        if step == 1:
            return self.row % 2 == 1
        held, _ = self.shared(step)
        return held == 0

    def apart(self, step):
        held, count = self.shared(step)
        return (held > 0) & (held < count)


def tiles(vol_q, unit):
    count = vol_q // unit
    groups = [list(range(count - 3)), [count - 3, count - 2, count - 1]]
    depths = [3 * unit * len(steps) for steps in groups] + [4 * QP]
    flux_at = [0, depths[0], depths[0] + depths[1]]
    tests_at = [0]
    for depth in depths:
        tests_at.append(tests_at[-1] + (depth + 127) // 128 * 128)
    return groups, depths, flux_at, tests_at


def one_hot(shape, hit):
    row_id = lax.broadcasted_iota(jnp.int32, shape, 0)
    col_id = lax.broadcasted_iota(jnp.int32, shape, 1)
    return jnp.where(hit(row_id, col_id), 1.0, 0.0).astype(BF16)


def kernel(
    rows,
    cols,
    state_in,
    geometry,
    material_in,
    neighbours_in,
    send_in,
    vol_eval_in,
    vol_grad_in,
    face_eval_in,
    face_lift_in,
    normals_in,
    areas_in,
    out,
    state,
    material,
    neighbours,
    send_faces,
    vol_eval,
    vol_grad,
    face_eval,
    face_lift,
    normals,
    areas,
    metric,
    state_low,
    traces,
    turned,
    outgoing,
    pool,
    gathered,
    points,
    fluxes,
    tests,
    normal_rows,
    area_rows,
    own_flux,
    pick,
    far,
    load_sem,
    geo_send,
    geo_recv,
    face_send,
    face_recv,
    row_in,
    col_in,
    metric_by_row=None,
):
    row = lax.axis_index("row")
    col = lax.axis_index("col")
    quantities, basis, elems = state.shape
    local_q = geometry.shape[1]
    vol_q = vol_eval.shape[1]
    face_q = face_eval.shape[0]
    slots = send_faces.shape[2]
    direct = local_q % 16 == 0
    unit = max(local_q, 16)
    groups, depths, flux_at, tests_at = tiles(vol_q, unit)
    paired = rows & (rows - 1) == 0

    barrier = pltpu.get_barrier_semaphore()
    ordered = paired and rows > 1
    if ordered:
        order = Order(row, rows)
        for step in range(1, rows):

            @pl.when(order.later(step))
            def _():
                pl.semaphore_signal(
                    barrier,
                    inc=1,
                    device_id={"row": partner(row, step, rows)},
                    device_id_type=MESH,
                )

        for other in range(1, cols):

            @pl.when(col < other)
            def _():
                pl.semaphore_signal(barrier, inc=1, device_id={"col": other}, device_id_type=MESH)
    else:
        for step in range(1, rows):
            pl.semaphore_signal(
                barrier, inc=1, device_id={"row": lax.rem(row + step, rows)}, device_id_type=MESH
            )
        for step in range(1, cols):
            pl.semaphore_signal(
                barrier, inc=1, device_id={"col": lax.rem(col + step, cols)}, device_id_type=MESH
            )
    loads = {}
    groups_of_loads = [
        [
            (face_eval_in, face_eval),
            (state_in, state),
            (material_in, material),
            (neighbours_in, neighbours),
            (send_in, send_faces),
        ],
        [
            (vol_eval_in, vol_eval),
            (normals_in, normals),
            (areas_in, areas),
            (vol_grad_in, vol_grad),
            (face_lift_in, face_lift),
        ],
    ]
    for index, group in enumerate(groups_of_loads):
        loads[index] = [
            pltpu.make_async_copy(source, target, load_sem.at[index]) for source, target in group
        ]
        for copy in loads[index]:
            copy.start()
    own_copy = pltpu.make_async_copy(
        geometry.at[:, :, pl.ds(pl.multiple_of(row * elems, 128), elems)],
        metric.at[0],
        geo_recv.at[0],
    )
    own_copy.start()
    def geo_copy(step):
        peer = partner(row, step, rows) if paired else lax.rem(row + step, rows)
        return pltpu.make_async_remote_copy(
            src_ref=geometry.at[:, :, pl.ds(pl.multiple_of(peer * elems, 128), elems)],
            dst_ref=metric.at[step],
            send_sem=geo_send,
            recv_sem=geo_recv.at[step],
            device_id={"row": peer},
            device_id_type=MESH,
        )

    def face_copy(step):
        peer = lax.rem(col + step, cols)
        return pltpu.make_async_remote_copy(
            src_ref=outgoing.at[peer],
            dst_ref=pool.at[col],
            send_sem=face_send,
            recv_sem=face_recv,
            device_id={"col": peer},
            device_id_type=MESH,
        )

    def later_sends(steps, where=True):
        for step in steps:

            @pl.when(order.later(step) & where)
            def _():
                pl.semaphore_wait(row_in.at[step - 1], 1)
                geo_copies[step].start()

    geo_copies = [own_copy] + [geo_copy(step) for step in range(1, rows)]
    if ordered:
        due = col + sum(jnp.where(order.earlier(step), 1, 0) for step in range(1, rows))

        @pl.when(due > 0)
        def _():
            pl.semaphore_wait(barrier, due)

        for step in range(1, rows):

            @pl.when(order.earlier(step))
            def _():
                pl.semaphore_signal(
                    row_in.at[step - 1],
                    inc=1,
                    device_id={"row": partner(row, step, rows)},
                    device_id_type=MESH,
                )

        for step in range(1, rows):

            @pl.when(order.earlier(step))
            def _():
                geo_copies[step].start()

        for step in range(1, cols):

            @pl.when(col >= step)
            def _():
                pl.semaphore_signal(
                    col_in.at[step - 1], inc=1, device_id={"col": col - step}, device_id_type=MESH
                )

    else:
        pl.semaphore_wait(barrier, rows + cols - 2)
        for step in range(1, rows):
            geo_copies[step].start()

    wire = pool.shape[2]
    pool[col] = jnp.zeros((slots, wire), BF16)

    def turning_rows(r, c):
        f = r // (3 * QP)
        turn_id = r // QP - 3 * f
        q = r % QP
        k = q % 3
        moved = k + turn_id
        moved = jnp.where(moved >= 3, moved - 3, moved)
        return (c == (q - k + moved) * 4 + f) & (q < face_q)

    turning = one_hot((12 * QP, 4 * face_q), turning_rows)
    same = one_hot((slots, slots), lambda r, c: r == c)
    narrow = one_hot(
        (quantities * QP, wire),
        lambda r, c: (c == (r // QP) * (face_q + 1) + r % QP) & (r % QP <= face_q),
    )
    for copy in loads[0]:
        copy.wait()
    listed = send_faces[0]
    listed_face = listed // elems
    listed_elem = listed - listed_face * elems
    face_col = dot(same, listed_face.astype(F32).astype(BF16), 1, 1)
    elem_col = dot(same, listed_elem.astype(F32).astype(BF16), 1, 1)
    listed_col = (face_col * float(elems) + elem_col).astype(jnp.int32)
    face_ids = lax.broadcasted_iota(jnp.int32, (slots, 4 * elems), 1)
    send_pick = jnp.concatenate(
        [
            jnp.where(face_ids == listed_col[:, p : p + 1], 1.0, 0.0).astype(BF16)
            for p in range(cols)
        ],
        axis=0,
    )
    flat = face_eval[...].reshape(4 * face_q, basis).astype(BF16)
    face_basis = dot(turning, flat).astype(BF16)
    for m in range(quantities):
        state_low[m] = state[m].astype(BF16)
    kind = neighbours[0]
    peer_index = neighbours[1]
    target = neighbours[2]
    turn = neighbours[3]
    row_ids = lax.broadcasted_iota(jnp.int32, (QP, elems), 0)
    low_rows = []
    for i in range(3):
        low_rows.append(material[i : i + 1, :].astype(BF16).astype(F32))
    for i in range(3):
        low_rows.append(material[i : i + 1, :] - low_rows[i])

    for m in range(quantities):
        found = dot(face_basis, state_low[m])
        for f in range(4):
            zero = found[3 * f * QP : (3 * f + 1) * QP]
            one = found[(3 * f + 1) * QP : (3 * f + 2) * QP]
            two = found[(3 * f + 2) * QP : (3 * f + 3) * QP]
            traces[m, f * QP : (f + 1) * QP, :] = zero
            side = turn[f : f + 1]
            chosen = jnp.where(side == 0, zero, jnp.where(side == 1, two, one))
            if m < 6:
                chosen = jnp.where(row_ids == face_q, low_rows[m], chosen)
            turned[m * QP : (m + 1) * QP, f * elems : (f + 1) * elems] = chosen.astype(BF16)

    if ordered:
        later_sends(range(1, rows - 2), (row >= 2) | (col == 0))
        later_sends(range(rows - 2, rows), row >= 2)
        for step in range(1, rows):
            if (step // 2) & (step // 2 - 1):

                @pl.when(order.apart(step))
                def _():
                    geo_copies[step].start()

    listed_traces = dot(send_pick, turned[...], 1, 1).astype(BF16)
    listed_traces = dot(listed_traces, narrow).astype(BF16)
    for p in range(cols):
        outgoing[p] = listed_traces[p * slots : (p + 1) * slots]

    face_copies = [face_copy(step) for step in range(1, cols)]
    for step in range(1, cols):
        if ordered:

            @pl.when(col + step >= cols)
            def _():
                face_copies[step - 1].start()
        else:
            face_copies[step - 1].start()

    if ordered:
        later_sends(range(1, rows - 2), (row < 2) & (col > 0))
        later_sends(range(rows - 2, rows), row < 2)

    for copy in loads[1]:
        copy.wait()
    same_q = one_hot((vol_q, vol_q), lambda r, c: r == c)
    vol_basis = dot(same_q, vol_eval[...].astype(BF16), 1, 1).astype(BF16)
    for m in range(quantities):
        points[m] = dot(vol_basis, state_low[m])

    if ordered:
        for step in range(1, cols):

            @pl.when(col + step < cols)
            def _():
                pl.semaphore_wait(col_in.at[step - 1], 1)
                face_copies[step - 1].start()

    elem_ids = lax.broadcasted_iota(jnp.int32, (elems, elems), 0).astype(F32).astype(BF16)
    one_low = jnp.ones((elems, elems), BF16)
    zero_low = jnp.zeros((elems, elems), BF16)
    for f in range(4):
        source = target[f : f + 1]
        near = kind[f : f + 1] == 0
        for g in range(4):
            hit = near & (source >= g * elems) & (source < (g + 1) * elems)
            wanted = jnp.where(hit, source - g * elems, -1).astype(F32).astype(BF16)
            pick[g * elems : (g + 1) * elems, :] = jnp.where(elem_ids == wanted, one_low, zero_low)
        gathered[:, f * elems : (f + 1) * elems] = dot(turned[...], pick[...])

    spread = one_hot(
        (4 * QP, 4 * face_q), lambda r, c: (c == (r % QP) * 4 + r // QP) & (r % QP < face_q)
    )
    for i in range(3):
        flat = normals[i].astype(F32).reshape(4 * face_q, elems).astype(BF16)
        normal_rows[i] = dot(spread, flat)
    flat = areas[...].reshape(4 * face_q, elems)
    high = flat.astype(BF16)
    low = (flat - high.astype(F32)).astype(BF16)
    area_rows[...] = dot(spread, high) + dot(spread, low)


    for t, steps in enumerate(groups):
        wide = len(steps) * unit

        def sent_point(k, c):
            step = steps[0] + c // unit
            sender = partner(row, step, rows) if direct else step
            return k == sender * unit + c % unit

        chosen_q = one_hot((vol_q, wide), sent_point)
        for d in range(3):
            at = tests_at[t] + d * wide
            tests[:, at : at + wide] = dot(vol_grad[d], chosen_q).astype(BF16)
    flat = face_lift[...].reshape(4 * face_q, basis).astype(BF16)
    place = one_hot(
        (4 * face_q, 4 * QP),
        lambda r, c: (r == (c % QP) * 4 + c // QP) & (c % QP < face_q),
    )
    at = tests_at[2]
    tests[:, at : at + 4 * QP] = (-dot(flat, place, 0, 0)).astype(BF16)

    lame = material[0:1, :]
    rigid = material[1:2, :]
    light = material[2:3, :]

    def volume_part(step, start, count, read):
        t = [step in steps for steps in groups].index(True)
        wide = len(groups[t]) * unit
        base = flux_at[t] + (step - groups[t][0]) * unit
        for half in range(elems // 128):
            cut = slice(half * 128, (half + 1) * 128)
            values = [points[m, pl.ds(start, count), cut] for m in range(9)]
            press = [-lame[:, cut] * values[6 + i] for i in range(3)]
            shear = [-rigid[:, cut] * values[6 + i] for i in range(3)]
            force = [-light[:, cut] * values[i] for i in range(6)]
            for d in range(3):
                n = [read(3 * d + i, cut) for i in range(3)]
                results = normal_flux(press, shear, force, n)
                at = base + d * wide
                for m in range(9):
                    fluxes[m, at : at + count, cut] = results[m].astype(BF16)

    def arrived(step):
        if step == 0:
            own_copy.wait()
        else:
            geo_copies[step].wait_recv()

    def volume(steps):
        if direct:
            for step in steps:
                arrived(step)
                sender = partner(row, step, rows)
                volume_part(
                    step,
                    pl.multiple_of(sender * local_q, local_q),
                    local_q,
                    lambda k, cut: metric[step, k, :, cut].astype(F32),
                )
        else:
            if steps[0] == 0:
                for step in range(rows):
                    arrived(step)
                    metric_by_row[partner(row, step, rows)] = metric[step].astype(F32)
            group = 16 // local_q
            for block in steps:
                volume_part(
                    block,
                    block * 16,
                    16,
                    lambda k, cut: jnp.concatenate(
                        [metric_by_row[block * group + j, k, :, cut] for j in range(group)], axis=0
                    ),
                )

    def contract(t, m):
        left = tests[:, tests_at[t] : tests_at[t] + depths[t]]
        return dot(left, fluxes[m, flux_at[t] : flux_at[t] + depths[t], :])

    pool_ids = lax.broadcasted_iota(jnp.int32, (cols * slots, elems), 0)
    for f in range(4):
        wanted = jnp.where(
            kind[f : f + 1] == 1, peer_index[f : f + 1] * slots + target[f : f + 1], -1
        )
        far[:, f * elems : (f + 1) * elems] = jnp.where(pool_ids == wanted, 1.0, 0.0).astype(BF16)
    own_speed = jnp.sqrt((lame + 2.0 * rigid) * light)

    def face_parts(f):
        for half in range(elems // 128):
            for part in range(QP // 16):
                yield slice(half * 128, (half + 1) * 128), f * QP + part * 16, part * 16

    def own_face(f):
        free = jnp.where(kind[f : f + 1] == 2, 1.0, 0.0)
        for cut, at, part in face_parts(f):
            a0, a1, a2 = -0.5 * lame[:, cut], -0.5 * rigid[:, cut], -0.5 * light[:, cut]
            n = [normal_rows[i, at : at + 16, cut] for i in range(3)]
            own = [traces[m, at : at + 16, cut] for m in range(9)]
            results = normal_flux(
                [a0 * own[6 + i] for i in range(3)],
                [a1 * own[6 + i] for i in range(3)],
                [a2 * own[i] for i in range(6)],
                n,
            )
            left = f * elems + cut.start
            for m in range(9):
                own_flux[m, at : at + 16, cut] = results[m]
                top = m * QP + part
                part_own = free[:, cut] * own[m]
                value = gathered[top : top + 16, left : left + 128]
                gathered[top : top + 16, left : left + 128] = (
                    value - part_own if m < 6 else value + part_own
                )

    def surface_face(f):
        lanes = slice(f * elems, (f + 1) * elems)
        edge = jnp.where(kind[f : f + 1] >= 2, 1.0, 0.0)
        other = []
        for i in range(3):
            high_at = i * QP + face_q
            low_at = (i + 3) * QP + face_q
            other.append(
                gathered[high_at : high_at + 1, lanes]
                + gathered[low_at : low_at + 1, lanes]
                + edge * material[i : i + 1, :]
            )
        speed = jnp.sqrt((other[0] + 2.0 * other[1]) * other[2])
        penalty_scale = 0.5 * jnp.maximum(own_speed, speed)
        for cut, at, part in face_parts(f):
            b0, b1, b2 = -0.5 * other[0][:, cut], -0.5 * other[1][:, cut], -0.5 * other[2][:, cut]
            n = [normal_rows[i, at : at + 16, cut] for i in range(3)]
            pen = penalty_scale[:, cut] * area_rows[at : at + 16, cut]
            left = f * elems + cut.start
            met = [gathered[m * QP + part : m * QP + part + 16, left : left + 128] for m in range(9)]
            results = normal_flux(
                [b0 * met[6 + i] for i in range(3)],
                [b1 * met[6 + i] for i in range(3)],
                [b2 * met[i] for i in range(6)],
                n,
            )
            to = flux_at[2] + at
            for m in range(9):
                gap = traces[m, at : at + 16, cut] - met[m]
                total = own_flux[m, at : at + 16, cut] + results[m] + pen * gap
                fluxes[m, to : to + 16, cut] = total.astype(BF16)

    factor = material[3:4, :]
    for f in range(4):
        own_face(f)
    volume(groups[0])
    for m in range(quantities):
        out[m] = contract(0, m)
    whole = pool.at[pl.ds(0, cols - 1)]
    pltpu.make_async_copy(whole, whole, face_recv).wait()
    received = pool[...].reshape(cols * slots, wire)
    received = dot(narrow, received, 1, 1).astype(BF16)
    gathered[...] = gathered[...] + dot(received, far[...])
    for f in range(4):
        surface_face(f)
    for m in range(quantities):
        out[m] = out[m] + contract(2, m)
    volume(groups[1])
    whole = metric.at[pl.ds(0, rows - 1)]
    pltpu.make_async_copy(whole, whole, geo_send).wait()
    whole = outgoing.at[pl.ds(0, cols - 1)]
    pltpu.make_async_copy(whole, whole, face_send).wait()
    for m in range(quantities):
        out[m] = state[m] + factor * (out[m] + contract(1, m))


def normal_flux(press, shear, force, n):
    pressure = press[0] * n[0] + press[1] * n[1] + press[2] * n[2]
    twice = [shear[i] + shear[i] for i in range(3)]
    return [
        pressure + twice[0] * n[0],
        pressure + twice[1] * n[1],
        pressure + twice[2] * n[2],
        n[0] * shear[1] + n[1] * shear[0],
        n[1] * shear[2] + n[2] * shear[1],
        n[0] * shear[2] + n[2] * shear[0],
        force[0] * n[0] + force[3] * n[1] + force[5] * n[2],
        force[3] * n[0] + force[1] * n[1] + force[4] * n[2],
        force[5] * n[0] + force[4] * n[1] + force[2] * n[2],
    ]


def per_device(
    rows,
    cols,
    state,
    geometry,
    material,
    neighbours,
    send_faces,
    vol_eval,
    vol_grad,
    face_eval,
    face_lift,
    normals,
    areas,
):
    quantities, basis, elems = state.shape
    slots = send_faces.shape[2]
    vol_q = vol_eval.shape[1]
    local_q = geometry.shape[1]
    total = 3 * vol_q + 4 * QP
    wire = (quantities * (face_eval.shape[2] + 1) + 127) // 128 * 128
    tests_at = tiles(vol_q, max(local_q, 16))[3]
    operands = [
        state,
        geometry,
        material,
        neighbours,
        send_faces,
        vol_eval,
        vol_grad,
        jnp.transpose(face_eval, (2, 0, 1)),
        jnp.transpose(face_lift, (2, 0, 1)),
        normals,
        areas,
    ]
    staged = [pltpu.VMEM(x.shape, x.dtype) for x in operands[:1] + operands[2:]]
    scratch = staged + [
        pltpu.VMEM((rows, 9, local_q, elems), BF16),
        pltpu.VMEM((quantities, basis, elems), BF16),
        pltpu.VMEM((quantities, 4 * QP, elems), F32),
        pltpu.VMEM((quantities * QP, 4 * elems), BF16),
        pltpu.VMEM((cols, slots, wire), BF16),
        pltpu.VMEM((cols, slots, wire), BF16),
        pltpu.VMEM((quantities * QP, 4 * elems), F32),
        pltpu.VMEM((quantities, vol_q, elems), F32),
        pltpu.VMEM((quantities, total, elems), BF16),
        pltpu.VMEM((basis, tests_at[-1]), BF16),
        pltpu.VMEM((3, 4 * QP, elems), F32),
        pltpu.VMEM((4 * QP, elems), F32),
        pltpu.VMEM((quantities, 4 * QP, elems), F32),
        pltpu.VMEM((4 * elems, elems), BF16),
        pltpu.VMEM((cols * slots, 4 * elems), BF16),
        pltpu.SemaphoreType.DMA((2,)),
        pltpu.SemaphoreType.DMA,
        pltpu.SemaphoreType.DMA((rows,)),
        pltpu.SemaphoreType.DMA,
        pltpu.SemaphoreType.DMA,
        pltpu.SemaphoreType.REGULAR((rows - 1,)),
        pltpu.SemaphoreType.REGULAR((cols - 1,)),
    ]
    if local_q % 16 != 0:
        scratch.append(pltpu.VMEM((rows, 9, local_q, elems), F32))
    return pl.pallas_call(
        functools.partial(kernel, rows, cols),
        out_shape=jax.ShapeDtypeStruct(state.shape, F32),
        in_specs=[pl.BlockSpec(memory_space=pltpu.HBM)] * len(operands),
        out_specs=pl.BlockSpec(memory_space=pltpu.VMEM),
        scratch_shapes=scratch,
        compiler_params=pltpu.CompilerParams(
            collective_id=0, has_side_effects=True, vmem_limit_bytes=48 * 1024 * 1024
        ),
    )(*[pltpu.with_memory_space_constraint(x, pltpu.HBM) for x in operands])


def solution(mesh):
    return jax.shard_map(
        functools.partial(per_device, mesh.shape["row"], mesh.shape["col"]),
        mesh=mesh,
        in_specs=(
            P(None, None, ("col", "row")),
            P(None, "row", "col"),
            P(None, ("col", "row")),
            P(None, None, ("col", "row")),
            P(("col", "row"), None, None),
            P(),
            P(),
            P(),
            P(),
            P(None, None, None, ("col", "row")),
            P(None, None, ("col", "row")),
        ),
        out_specs=P(None, None, ("col", "row")),
        check_vma=False,
    )
```

```python
import functools

import jax
import jax.numpy as jnp
from jax import lax
from jax.experimental import pallas as pl
from jax.experimental.pallas import tpu as pltpu
from jax.sharding import PartitionSpec as P

F32 = jnp.float32
BF16 = jnp.bfloat16
QP = 32
MESH = pl.DeviceIdType.MESH


def dot(left, right, left_dim=1, right_dim=0):
    return lax.dot_general(
        left, right, (((left_dim,), (right_dim,)), ((), ())), preferred_element_type=F32
    )


def partner(row, step, rows):
    if rows & (rows - 1):
        other = row - step
        return other + jnp.where(other < 0, rows, 0)
    total, bit = 0, 1
    while bit < rows:
        total = total + ((row // bit + step // bit) % 2) * bit
        bit *= 2
    return total


class Order:
    def __init__(self, row, rows):
        self.row, self.rows = row, rows

    def shared(self, step):
        bits = [b for b in range(1, self.rows.bit_length()) if (step >> b) & 1]
        return sum((self.row // (1 << b)) % 2 for b in bits), len(bits)

    def earlier(self, step):
        if step == 1:
            return self.row % 2 == 0
        held, count = self.shared(step)
        return held == count

    def later(self, step):
        if step == 1:
            return self.row % 2 == 1
        held, _ = self.shared(step)
        return held == 0

    def apart(self, step):
        held, count = self.shared(step)
        return (held > 0) & (held < count)


def tiles(vol_q, unit):
    count = vol_q // unit
    groups = [list(range(count - 3)), [count - 3, count - 2, count - 1]]
    depths = [3 * unit * len(steps) for steps in groups] + [4 * QP]
    flux_at = [0, depths[0], depths[0] + depths[1]]
    tests_at = [0]
    for depth in depths:
        tests_at.append(tests_at[-1] + (depth + 127) // 128 * 128)
    return groups, depths, flux_at, tests_at


def one_hot(shape, hit):
    row_id = lax.broadcasted_iota(jnp.int32, shape, 0)
    col_id = lax.broadcasted_iota(jnp.int32, shape, 1)
    return jnp.where(hit(row_id, col_id), 1.0, 0.0).astype(BF16)


def kernel(
    rows,
    cols,
    state_in,
    geometry,
    material_in,
    neighbours_in,
    send_in,
    vol_eval_in,
    vol_grad_in,
    face_eval_in,
    face_lift_in,
    normals_in,
    areas_in,
    out,
    state,
    material,
    neighbours,
    send_faces,
    vol_eval,
    vol_grad,
    face_eval,
    face_lift,
    normals,
    areas,
    metric,
    state_low,
    traces,
    turned,
    outgoing,
    pool,
    gathered,
    points,
    fluxes,
    tests,
    normal_rows,
    area_rows,
    own_flux,
    pick,
    far,
    load_sem,
    geo_send,
    geo_recv,
    face_send,
    face_recv,
    row_in,
    col_in,
    metric_by_row=None,
):
    row = lax.axis_index("row")
    col = lax.axis_index("col")
    quantities, basis, elems = state.shape
    local_q = geometry.shape[1]
    vol_q = vol_eval.shape[1]
    face_q = face_eval.shape[0]
    slots = send_faces.shape[2]
    direct = local_q % 16 == 0
    unit = max(local_q, 16)
    groups, depths, flux_at, tests_at = tiles(vol_q, unit)
    paired = rows & (rows - 1) == 0

    barrier = pltpu.get_barrier_semaphore()
    ordered = paired and rows > 1
    if ordered:
        order = Order(row, rows)
        for step in range(1, rows):

            @pl.when(order.later(step))
            def _():
                pl.semaphore_signal(
                    barrier,
                    inc=1,
                    device_id={"row": partner(row, step, rows)},
                    device_id_type=MESH,
                )

        for other in range(1, cols):

            @pl.when(col < other)
            def _():
                pl.semaphore_signal(barrier, inc=1, device_id={"col": other}, device_id_type=MESH)
    else:
        for step in range(1, rows):
            pl.semaphore_signal(
                barrier, inc=1, device_id={"row": lax.rem(row + step, rows)}, device_id_type=MESH
            )
        for step in range(1, cols):
            pl.semaphore_signal(
                barrier, inc=1, device_id={"col": lax.rem(col + step, cols)}, device_id_type=MESH
            )
    loads = {}
    groups_of_loads = [
        [
            (face_eval_in, face_eval),
            (state_in, state),
            (material_in, material),
            (neighbours_in, neighbours),
            (send_in, send_faces),
        ],
        [
            (vol_eval_in, vol_eval),
            (normals_in, normals),
            (areas_in, areas),
            (vol_grad_in, vol_grad),
            (face_lift_in, face_lift),
        ],
    ]
    for index, group in enumerate(groups_of_loads):
        loads[index] = [
            pltpu.make_async_copy(source, target, load_sem.at[index]) for source, target in group
        ]
        for copy in loads[index]:
            copy.start()
    own_copy = pltpu.make_async_copy(
        geometry.at[:, :, pl.ds(pl.multiple_of(row * elems, 128), elems)],
        metric.at[0],
        geo_recv.at[0],
    )
    own_copy.start()
    def geo_copy(step):
        peer = partner(row, step, rows) if paired else lax.rem(row + step, rows)
        return pltpu.make_async_remote_copy(
            src_ref=geometry.at[:, :, pl.ds(pl.multiple_of(peer * elems, 128), elems)],
            dst_ref=metric.at[step],
            send_sem=geo_send,
            recv_sem=geo_recv.at[step],
            device_id={"row": peer},
            device_id_type=MESH,
        )

    def face_copy(step):
        peer = lax.rem(col + step, cols)
        return pltpu.make_async_remote_copy(
            src_ref=outgoing.at[peer],
            dst_ref=pool.at[col],
            send_sem=face_send,
            recv_sem=face_recv,
            device_id={"col": peer},
            device_id_type=MESH,
        )

    def later_sends(steps, where=True):
        for step in steps:

            @pl.when(order.later(step) & where)
            def _():
                pl.semaphore_wait(row_in.at[step - 1], 1)
                geo_copies[step].start()

    geo_copies = [own_copy] + [geo_copy(step) for step in range(1, rows)]
    if ordered:
        due = col + sum(jnp.where(order.earlier(step), 1, 0) for step in range(1, rows))

        @pl.when(due > 0)
        def _():
            pl.semaphore_wait(barrier, due)

        for step in range(1, rows):

            @pl.when(order.earlier(step))
            def _():
                pl.semaphore_signal(
                    row_in.at[step - 1],
                    inc=1,
                    device_id={"row": partner(row, step, rows)},
                    device_id_type=MESH,
                )

        far_first = sorted(range(1, rows), key=lambda step: (-(step // 2), step))
        for core, steps in ((0, range(1, rows)), (1, far_first)):
            for step in steps:

                @pl.when(order.earlier(step) & (row % 2 == core))
                def _():
                    geo_copies[step].start()

        for step in range(1, cols):

            @pl.when(col >= step)
            def _():
                pl.semaphore_signal(
                    col_in.at[step - 1], inc=1, device_id={"col": col - step}, device_id_type=MESH
                )

    else:
        pl.semaphore_wait(barrier, rows + cols - 2)
        for step in range(1, rows):
            geo_copies[step].start()

    wire = pool.shape[2]
    pool[col] = jnp.zeros((slots, wire), BF16)

    def turning_rows(r, c):
        f = r // (3 * QP)
        turn_id = r // QP - 3 * f
        q = r % QP
        k = q % 3
        moved = k + turn_id
        moved = jnp.where(moved >= 3, moved - 3, moved)
        return (c == (q - k + moved) * 4 + f) & (q < face_q)

    turning = one_hot((12 * QP, 4 * face_q), turning_rows)
    same = one_hot((slots, slots), lambda r, c: r == c)
    narrow = one_hot(
        (quantities * QP, wire),
        lambda r, c: (c == (r // QP) * (face_q + 1) + r % QP) & (r % QP <= face_q),
    )
    for copy in loads[0]:
        copy.wait()
    listed = send_faces[0]
    listed_face = listed // elems
    listed_elem = listed - listed_face * elems
    face_col = dot(same, listed_face.astype(F32).astype(BF16), 1, 1)
    elem_col = dot(same, listed_elem.astype(F32).astype(BF16), 1, 1)
    listed_col = (face_col * float(elems) + elem_col).astype(jnp.int32)
    face_ids = lax.broadcasted_iota(jnp.int32, (slots, 4 * elems), 1)
    send_pick = jnp.concatenate(
        [
            jnp.where(face_ids == listed_col[:, p : p + 1], 1.0, 0.0).astype(BF16)
            for p in range(cols)
        ],
        axis=0,
    )
    flat = face_eval[...].reshape(4 * face_q, basis).astype(BF16)
    face_basis = dot(turning, flat).astype(BF16)
    for m in range(quantities):
        state_low[m] = state[m].astype(BF16)
    kind = neighbours[0]
    peer_index = neighbours[1]
    target = neighbours[2]
    turn = neighbours[3]
    row_ids = lax.broadcasted_iota(jnp.int32, (QP, elems), 0)
    low_rows = []
    for i in range(3):
        low_rows.append(material[i : i + 1, :].astype(BF16).astype(F32))
    for i in range(3):
        low_rows.append(material[i : i + 1, :] - low_rows[i])

    for m in range(quantities):
        found = dot(face_basis, state_low[m])
        for f in range(4):
            zero = found[3 * f * QP : (3 * f + 1) * QP]
            one = found[(3 * f + 1) * QP : (3 * f + 2) * QP]
            two = found[(3 * f + 2) * QP : (3 * f + 3) * QP]
            traces[m, f * QP : (f + 1) * QP, :] = zero
            side = turn[f : f + 1]
            chosen = jnp.where(side == 0, zero, jnp.where(side == 1, two, one))
            if m < 6:
                chosen = jnp.where(row_ids == face_q, low_rows[m], chosen)
            turned[m * QP : (m + 1) * QP, f * elems : (f + 1) * elems] = chosen.astype(BF16)

    if ordered:
        later_sends(range(1, rows - 2), (row >= 2) | (col == 0))
        later_sends(range(rows - 2, rows), row >= 2)
        for step in range(1, rows):
            if (step // 2) & (step // 2 - 1):

                @pl.when(order.apart(step))
                def _():
                    geo_copies[step].start()

    listed_traces = dot(send_pick, turned[...], 1, 1).astype(BF16)
    listed_traces = dot(listed_traces, narrow).astype(BF16)
    for p in range(cols):
        outgoing[p] = listed_traces[p * slots : (p + 1) * slots]

    face_copies = [face_copy(step) for step in range(1, cols)]
    for step in range(1, cols):
        if ordered:

            @pl.when(col + step >= cols)
            def _():
                face_copies[step - 1].start()
        else:
            face_copies[step - 1].start()

    if ordered:
        later_sends(range(1, rows - 2), (row < 2) & (col > 0))
        later_sends(range(rows - 2, rows), row < 2)

    for copy in loads[1]:
        copy.wait()
    same_q = one_hot((vol_q, vol_q), lambda r, c: r == c)
    vol_basis = dot(same_q, vol_eval[...].astype(BF16), 1, 1).astype(BF16)
    for m in range(quantities):
        points[m] = dot(vol_basis, state_low[m])

    if ordered:
        for step in range(1, cols):

            @pl.when(col + step < cols)
            def _():
                pl.semaphore_wait(col_in.at[step - 1], 1)
                face_copies[step - 1].start()

    elem_ids = lax.broadcasted_iota(jnp.int32, (elems, elems), 0).astype(F32).astype(BF16)
    one_low = jnp.ones((elems, elems), BF16)
    zero_low = jnp.zeros((elems, elems), BF16)
    for f in range(4):
        source = target[f : f + 1]
        near = kind[f : f + 1] == 0
        for g in range(4):
            hit = near & (source >= g * elems) & (source < (g + 1) * elems)
            wanted = jnp.where(hit, source - g * elems, -1).astype(F32).astype(BF16)
            pick[g * elems : (g + 1) * elems, :] = jnp.where(elem_ids == wanted, one_low, zero_low)
        gathered[:, f * elems : (f + 1) * elems] = dot(turned[...], pick[...])

    spread = one_hot(
        (4 * QP, 4 * face_q), lambda r, c: (c == (r % QP) * 4 + r // QP) & (r % QP < face_q)
    )
    for i in range(3):
        flat = normals[i].astype(F32).reshape(4 * face_q, elems).astype(BF16)
        normal_rows[i] = dot(spread, flat)
    flat = areas[...].reshape(4 * face_q, elems)
    high = flat.astype(BF16)
    low = (flat - high.astype(F32)).astype(BF16)
    area_rows[...] = dot(spread, high) + dot(spread, low)


    for t, steps in enumerate(groups):
        wide = len(steps) * unit

        def sent_point(k, c):
            step = steps[0] + c // unit
            sender = partner(row, step, rows) if direct else step
            return k == sender * unit + c % unit

        chosen_q = one_hot((vol_q, wide), sent_point)
        for d in range(3):
            at = tests_at[t] + d * wide
            tests[:, at : at + wide] = dot(vol_grad[d], chosen_q).astype(BF16)
    flat = face_lift[...].reshape(4 * face_q, basis).astype(BF16)
    place = one_hot(
        (4 * face_q, 4 * QP),
        lambda r, c: (r == (c % QP) * 4 + c // QP) & (c % QP < face_q),
    )
    at = tests_at[2]
    tests[:, at : at + 4 * QP] = (-dot(flat, place, 0, 0)).astype(BF16)

    lame = material[0:1, :]
    rigid = material[1:2, :]
    light = material[2:3, :]

    def volume_part(step, start, count, read):
        t = [step in steps for steps in groups].index(True)
        wide = len(groups[t]) * unit
        base = flux_at[t] + (step - groups[t][0]) * unit
        for half in range(elems // 128):
            cut = slice(half * 128, (half + 1) * 128)
            values = [points[m, pl.ds(start, count), cut] for m in range(9)]
            press = [-lame[:, cut] * values[6 + i] for i in range(3)]
            shear = [-rigid[:, cut] * values[6 + i] for i in range(3)]
            force = [-light[:, cut] * values[i] for i in range(6)]
            for d in range(3):
                n = [read(3 * d + i, cut) for i in range(3)]
                results = normal_flux(press, shear, force, n)
                at = base + d * wide
                for m in range(9):
                    fluxes[m, at : at + count, cut] = results[m].astype(BF16)

    def arrived(step):
        if step == 0:
            own_copy.wait()
        else:
            geo_copies[step].wait_recv()

    def volume(steps):
        if direct:
            for step in steps:
                arrived(step)
                sender = partner(row, step, rows)
                volume_part(
                    step,
                    pl.multiple_of(sender * local_q, local_q),
                    local_q,
                    lambda k, cut: metric[step, k, :, cut].astype(F32),
                )
        else:
            if steps[0] == 0:
                for step in range(rows):
                    arrived(step)
                    metric_by_row[partner(row, step, rows)] = metric[step].astype(F32)
            group = 16 // local_q
            for block in steps:
                volume_part(
                    block,
                    block * 16,
                    16,
                    lambda k, cut: jnp.concatenate(
                        [metric_by_row[block * group + j, k, :, cut] for j in range(group)], axis=0
                    ),
                )

    def contract(t, m):
        left = tests[:, tests_at[t] : tests_at[t] + depths[t]]
        return dot(left, fluxes[m, flux_at[t] : flux_at[t] + depths[t], :])

    pool_ids = lax.broadcasted_iota(jnp.int32, (cols * slots, elems), 0)
    for f in range(4):
        wanted = jnp.where(
            kind[f : f + 1] == 1, peer_index[f : f + 1] * slots + target[f : f + 1], -1
        )
        far[:, f * elems : (f + 1) * elems] = jnp.where(pool_ids == wanted, 1.0, 0.0).astype(BF16)
    own_speed = jnp.sqrt((lame + 2.0 * rigid) * light)

    def face_parts(f):
        for half in range(elems // 128):
            for part in range(QP // 16):
                yield slice(half * 128, (half + 1) * 128), f * QP + part * 16, part * 16

    def own_face(f):
        free = jnp.where(kind[f : f + 1] == 2, 1.0, 0.0)
        for cut, at, part in face_parts(f):
            a0, a1, a2 = -0.5 * lame[:, cut], -0.5 * rigid[:, cut], -0.5 * light[:, cut]
            n = [normal_rows[i, at : at + 16, cut] for i in range(3)]
            own = [traces[m, at : at + 16, cut] for m in range(9)]
            results = normal_flux(
                [a0 * own[6 + i] for i in range(3)],
                [a1 * own[6 + i] for i in range(3)],
                [a2 * own[i] for i in range(6)],
                n,
            )
            left = f * elems + cut.start
            for m in range(9):
                own_flux[m, at : at + 16, cut] = results[m]
                top = m * QP + part
                part_own = free[:, cut] * own[m]
                value = gathered[top : top + 16, left : left + 128]
                gathered[top : top + 16, left : left + 128] = (
                    value - part_own if m < 6 else value + part_own
                )

    def surface_face(f):
        lanes = slice(f * elems, (f + 1) * elems)
        edge = jnp.where(kind[f : f + 1] >= 2, 1.0, 0.0)
        other = []
        for i in range(3):
            high_at = i * QP + face_q
            low_at = (i + 3) * QP + face_q
            other.append(
                gathered[high_at : high_at + 1, lanes]
                + gathered[low_at : low_at + 1, lanes]
                + edge * material[i : i + 1, :]
            )
        speed = jnp.sqrt((other[0] + 2.0 * other[1]) * other[2])
        penalty_scale = 0.5 * jnp.maximum(own_speed, speed)
        for cut, at, part in face_parts(f):
            b0, b1, b2 = -0.5 * other[0][:, cut], -0.5 * other[1][:, cut], -0.5 * other[2][:, cut]
            n = [normal_rows[i, at : at + 16, cut] for i in range(3)]
            pen = penalty_scale[:, cut] * area_rows[at : at + 16, cut]
            left = f * elems + cut.start
            met = [gathered[m * QP + part : m * QP + part + 16, left : left + 128] for m in range(9)]
            results = normal_flux(
                [b0 * met[6 + i] for i in range(3)],
                [b1 * met[6 + i] for i in range(3)],
                [b2 * met[i] for i in range(6)],
                n,
            )
            to = flux_at[2] + at
            for m in range(9):
                gap = traces[m, at : at + 16, cut] - met[m]
                total = own_flux[m, at : at + 16, cut] + results[m] + pen * gap
                fluxes[m, to : to + 16, cut] = total.astype(BF16)

    factor = material[3:4, :]
    for f in range(4):
        own_face(f)
    volume(groups[0])
    for m in range(quantities):
        out[m] = contract(0, m)
    whole = pool.at[pl.ds(0, cols - 1)]
    pltpu.make_async_copy(whole, whole, face_recv).wait()
    received = pool[...].reshape(cols * slots, wire)
    received = dot(narrow, received, 1, 1).astype(BF16)
    gathered[...] = gathered[...] + dot(received, far[...])
    for f in range(4):
        surface_face(f)
    for m in range(quantities):
        out[m] = out[m] + contract(2, m)
    volume(groups[1])
    whole = metric.at[pl.ds(0, rows - 1)]
    pltpu.make_async_copy(whole, whole, geo_send).wait()
    whole = outgoing.at[pl.ds(0, cols - 1)]
    pltpu.make_async_copy(whole, whole, face_send).wait()
    for m in range(quantities):
        out[m] = state[m] + factor * (out[m] + contract(1, m))


def normal_flux(press, shear, force, n):
    pressure = press[0] * n[0] + press[1] * n[1] + press[2] * n[2]
    twice = [shear[i] + shear[i] for i in range(3)]
    return [
        pressure + twice[0] * n[0],
        pressure + twice[1] * n[1],
        pressure + twice[2] * n[2],
        n[0] * shear[1] + n[1] * shear[0],
        n[1] * shear[2] + n[2] * shear[1],
        n[0] * shear[2] + n[2] * shear[0],
        force[0] * n[0] + force[3] * n[1] + force[5] * n[2],
        force[3] * n[0] + force[1] * n[1] + force[4] * n[2],
        force[5] * n[0] + force[4] * n[1] + force[2] * n[2],
    ]


def per_device(
    rows,
    cols,
    state,
    geometry,
    material,
    neighbours,
    send_faces,
    vol_eval,
    vol_grad,
    face_eval,
    face_lift,
    normals,
    areas,
):
    quantities, basis, elems = state.shape
    slots = send_faces.shape[2]
    vol_q = vol_eval.shape[1]
    local_q = geometry.shape[1]
    total = 3 * vol_q + 4 * QP
    wire = (quantities * (face_eval.shape[2] + 1) + 127) // 128 * 128
    tests_at = tiles(vol_q, max(local_q, 16))[3]
    operands = [
        state,
        geometry,
        material,
        neighbours,
        send_faces,
        vol_eval,
        vol_grad,
        jnp.transpose(face_eval, (2, 0, 1)),
        jnp.transpose(face_lift, (2, 0, 1)),
        normals,
        areas,
    ]
    staged = [pltpu.VMEM(x.shape, x.dtype) for x in operands[:1] + operands[2:]]
    scratch = staged + [
        pltpu.VMEM((rows, 9, local_q, elems), BF16),
        pltpu.VMEM((quantities, basis, elems), BF16),
        pltpu.VMEM((quantities, 4 * QP, elems), F32),
        pltpu.VMEM((quantities * QP, 4 * elems), BF16),
        pltpu.VMEM((cols, slots, wire), BF16),
        pltpu.VMEM((cols, slots, wire), BF16),
        pltpu.VMEM((quantities * QP, 4 * elems), F32),
        pltpu.VMEM((quantities, vol_q, elems), F32),
        pltpu.VMEM((quantities, total, elems), BF16),
        pltpu.VMEM((basis, tests_at[-1]), BF16),
        pltpu.VMEM((3, 4 * QP, elems), F32),
        pltpu.VMEM((4 * QP, elems), F32),
        pltpu.VMEM((quantities, 4 * QP, elems), F32),
        pltpu.VMEM((4 * elems, elems), BF16),
        pltpu.VMEM((cols * slots, 4 * elems), BF16),
        pltpu.SemaphoreType.DMA((2,)),
        pltpu.SemaphoreType.DMA,
        pltpu.SemaphoreType.DMA((rows,)),
        pltpu.SemaphoreType.DMA,
        pltpu.SemaphoreType.DMA,
        pltpu.SemaphoreType.REGULAR((rows - 1,)),
        pltpu.SemaphoreType.REGULAR((cols - 1,)),
    ]
    if local_q % 16 != 0:
        scratch.append(pltpu.VMEM((rows, 9, local_q, elems), F32))
    return pl.pallas_call(
        functools.partial(kernel, rows, cols),
        out_shape=jax.ShapeDtypeStruct(state.shape, F32),
        in_specs=[pl.BlockSpec(memory_space=pltpu.HBM)] * len(operands),
        out_specs=pl.BlockSpec(memory_space=pltpu.VMEM),
        scratch_shapes=scratch,
        compiler_params=pltpu.CompilerParams(
            collective_id=0, has_side_effects=True, vmem_limit_bytes=48 * 1024 * 1024
        ),
    )(*[pltpu.with_memory_space_constraint(x, pltpu.HBM) for x in operands])


def solution(mesh):
    return jax.shard_map(
        functools.partial(per_device, mesh.shape["row"], mesh.shape["col"]),
        mesh=mesh,
        in_specs=(
            P(None, None, ("col", "row")),
            P(None, "row", "col"),
            P(None, ("col", "row")),
            P(None, None, ("col", "row")),
            P(("col", "row"), None, None),
            P(),
            P(),
            P(),
            P(),
            P(None, None, None, ("col", "row")),
            P(None, None, ("col", "row")),
        ),
        out_specs=P(None, None, ("col", "row")),
        check_vma=False,
    )
```

```python
import functools

import jax
import jax.numpy as jnp
from jax import lax
from jax.experimental import pallas as pl
from jax.experimental.pallas import tpu as pltpu
from jax.sharding import PartitionSpec as P

F32 = jnp.float32
BF16 = jnp.bfloat16
QP = 32
MESH = pl.DeviceIdType.MESH


def dot(left, right, left_dim=1, right_dim=0):
    return lax.dot_general(
        left, right, (((left_dim,), (right_dim,)), ((), ())), preferred_element_type=F32
    )


def partner(row, step, rows):
    if rows & (rows - 1):
        other = row - step
        return other + jnp.where(other < 0, rows, 0)
    total, bit = 0, 1
    while bit < rows:
        total = total + ((row // bit + step // bit) % 2) * bit
        bit *= 2
    return total


class Order:
    def __init__(self, row, rows):
        self.row, self.rows = row, rows

    def shared(self, step):
        bits = [b for b in range(1, self.rows.bit_length()) if (step >> b) & 1]
        return sum((self.row // (1 << b)) % 2 for b in bits), len(bits)

    def earlier(self, step):
        if step == 1:
            return self.row % 2 == 0
        held, count = self.shared(step)
        return held == count

    def later(self, step):
        if step == 1:
            return self.row % 2 == 1
        held, _ = self.shared(step)
        return held == 0

    def apart(self, step):
        held, count = self.shared(step)
        return (held > 0) & (held < count)


def tiles(vol_q, unit):
    count = vol_q // unit
    groups = [list(range(count - 3)), [count - 3, count - 2, count - 1]]
    depths = [3 * unit * len(steps) for steps in groups] + [4 * QP]
    flux_at = [0, depths[0], depths[0] + depths[1]]
    tests_at = [0]
    for depth in depths:
        tests_at.append(tests_at[-1] + (depth + 127) // 128 * 128)
    return groups, depths, flux_at, tests_at


def one_hot(shape, hit):
    row_id = lax.broadcasted_iota(jnp.int32, shape, 0)
    col_id = lax.broadcasted_iota(jnp.int32, shape, 1)
    return jnp.where(hit(row_id, col_id), 1.0, 0.0).astype(BF16)


def kernel(
    rows,
    cols,
    state_in,
    geometry,
    material_in,
    neighbours_in,
    send_in,
    vol_eval_in,
    vol_grad_in,
    face_eval_in,
    face_lift_in,
    normals_in,
    areas_in,
    out,
    state,
    material,
    neighbours,
    send_faces,
    vol_eval,
    vol_grad,
    face_eval,
    face_lift,
    normals,
    areas,
    metric,
    state_low,
    traces,
    turned,
    outgoing,
    pool,
    gathered,
    points,
    fluxes,
    tests,
    normal_rows,
    area_rows,
    own_flux,
    pick,
    far,
    load_sem,
    geo_send,
    geo_recv,
    face_send,
    face_recv,
    row_in,
    col_in,
    metric_by_row=None,
):
    row = lax.axis_index("row")
    col = lax.axis_index("col")
    quantities, basis, elems = state.shape
    local_q = geometry.shape[1]
    vol_q = vol_eval.shape[1]
    face_q = face_eval.shape[0]
    slots = send_faces.shape[2]
    direct = local_q % 16 == 0
    unit = max(local_q, 16)
    groups, depths, flux_at, tests_at = tiles(vol_q, unit)
    paired = rows & (rows - 1) == 0

    barrier = pltpu.get_barrier_semaphore()
    ordered = paired and rows > 1
    if ordered:
        order = Order(row, rows)
        for step in range(1, rows):

            @pl.when(order.later(step))
            def _():
                pl.semaphore_signal(
                    barrier,
                    inc=1,
                    device_id={"row": partner(row, step, rows)},
                    device_id_type=MESH,
                )

        for other in range(1, cols):

            @pl.when(col < other)
            def _():
                pl.semaphore_signal(barrier, inc=1, device_id={"col": other}, device_id_type=MESH)
    else:
        for step in range(1, rows):
            pl.semaphore_signal(
                barrier, inc=1, device_id={"row": lax.rem(row + step, rows)}, device_id_type=MESH
            )
        for step in range(1, cols):
            pl.semaphore_signal(
                barrier, inc=1, device_id={"col": lax.rem(col + step, cols)}, device_id_type=MESH
            )
    loads = {}
    groups_of_loads = [
        [
            (face_eval_in, face_eval),
            (state_in, state),
            (material_in, material),
            (neighbours_in, neighbours),
            (send_in, send_faces),
        ],
        [
            (vol_eval_in, vol_eval),
            (normals_in, normals),
            (areas_in, areas),
            (vol_grad_in, vol_grad),
            (face_lift_in, face_lift),
        ],
    ]
    for index, group in enumerate(groups_of_loads):
        loads[index] = [
            pltpu.make_async_copy(source, target, load_sem.at[index]) for source, target in group
        ]
        for copy in loads[index]:
            copy.start()
    own_copy = pltpu.make_async_copy(
        geometry.at[:, :, pl.ds(pl.multiple_of(row * elems, 128), elems)],
        metric.at[0],
        geo_recv.at[0],
    )
    own_copy.start()
    def geo_copy(step):
        peer = partner(row, step, rows) if paired else lax.rem(row + step, rows)
        return pltpu.make_async_remote_copy(
            src_ref=geometry.at[:, :, pl.ds(pl.multiple_of(peer * elems, 128), elems)],
            dst_ref=metric.at[step],
            send_sem=geo_send,
            recv_sem=geo_recv.at[step],
            device_id={"row": peer},
            device_id_type=MESH,
        )

    def face_copy(step):
        peer = lax.rem(col + step, cols)
        return pltpu.make_async_remote_copy(
            src_ref=outgoing.at[peer],
            dst_ref=pool.at[col],
            send_sem=face_send,
            recv_sem=face_recv,
            device_id={"col": peer},
            device_id_type=MESH,
        )

    def later_sends(steps, where=True):
        for step in steps:

            @pl.when(order.later(step) & where)
            def _():
                pl.semaphore_wait(row_in.at[step - 1], 1)
                geo_copies[step].start()

    geo_copies = [own_copy] + [geo_copy(step) for step in range(1, rows)]
    if ordered:
        due = col + sum(jnp.where(order.earlier(step), 1, 0) for step in range(1, rows))

        @pl.when(due > 0)
        def _():
            pl.semaphore_wait(barrier, due)

        for step in range(1, rows):

            @pl.when(order.earlier(step))
            def _():
                pl.semaphore_signal(
                    row_in.at[step - 1],
                    inc=1,
                    device_id={"row": partner(row, step, rows)},
                    device_id_type=MESH,
                )

        far_first = sorted(range(1, rows), key=lambda step: (-(step // 2), step))
        for core, steps in ((0, range(1, rows)), (1, far_first)):
            for step in steps:

                @pl.when(order.earlier(step) & (row % 2 == core))
                def _():
                    geo_copies[step].start()

        for step in range(1, cols):

            @pl.when(col >= step)
            def _():
                pl.semaphore_signal(
                    col_in.at[step - 1], inc=1, device_id={"col": col - step}, device_id_type=MESH
                )

    else:
        pl.semaphore_wait(barrier, rows + cols - 2)
        for step in range(1, rows):
            geo_copies[step].start()

    wire = pool.shape[2]
    pool[col] = jnp.zeros((slots, wire), BF16)

    def turning_rows(r, c):
        f = r // (3 * QP)
        turn_id = r // QP - 3 * f
        q = r % QP
        k = q % 3
        moved = k + turn_id
        moved = jnp.where(moved >= 3, moved - 3, moved)
        return (c == (q - k + moved) * 4 + f) & (q < face_q)

    turning = one_hot((12 * QP, 4 * face_q), turning_rows)
    same = one_hot((slots, slots), lambda r, c: r == c)
    narrow = one_hot(
        (quantities * QP, wire),
        lambda r, c: (c == (r // QP) * (face_q + 1) + r % QP) & (r % QP <= face_q),
    )
    for copy in loads[0]:
        copy.wait()
    listed = send_faces[0]
    listed_face = listed // elems
    listed_elem = listed - listed_face * elems
    face_col = dot(same, listed_face.astype(F32).astype(BF16), 1, 1)
    elem_col = dot(same, listed_elem.astype(F32).astype(BF16), 1, 1)
    listed_col = (face_col * float(elems) + elem_col).astype(jnp.int32)
    face_ids = lax.broadcasted_iota(jnp.int32, (slots, 4 * elems), 1)
    send_pick = jnp.concatenate(
        [
            jnp.where(face_ids == listed_col[:, p : p + 1], 1.0, 0.0).astype(BF16)
            for p in range(cols)
        ],
        axis=0,
    )
    flat = face_eval[...].reshape(4 * face_q, basis).astype(BF16)
    face_basis = dot(turning, flat).astype(BF16)
    for m in range(quantities):
        state_low[m] = state[m].astype(BF16)
    kind = neighbours[0]
    peer_index = neighbours[1]
    target = neighbours[2]
    turn = neighbours[3]
    row_ids = lax.broadcasted_iota(jnp.int32, (QP, elems), 0)
    low_rows = []
    for i in range(3):
        low_rows.append(material[i : i + 1, :].astype(BF16).astype(F32))
    for i in range(3):
        low_rows.append(material[i : i + 1, :] - low_rows[i])

    for m in range(quantities):
        found = dot(face_basis, state_low[m])
        for f in range(4):
            zero = found[3 * f * QP : (3 * f + 1) * QP]
            one = found[(3 * f + 1) * QP : (3 * f + 2) * QP]
            two = found[(3 * f + 2) * QP : (3 * f + 3) * QP]
            traces[m, f * QP : (f + 1) * QP, :] = zero
            side = turn[f : f + 1]
            chosen = jnp.where(side == 0, zero, jnp.where(side == 1, two, one))
            if m < 6:
                chosen = jnp.where(row_ids == face_q, low_rows[m], chosen)
            turned[m * QP : (m + 1) * QP, f * elems : (f + 1) * elems] = chosen.astype(BF16)

    if ordered:
        later_sends(range(1, rows - 2), (row >= 2) | (col == 0))
        later_sends(range(rows - 2, rows), row >= 2)
        for step in range(1, rows):
            if (step // 2) & (step // 2 - 1):

                @pl.when(order.apart(step))
                def _():
                    geo_copies[step].start()

    listed_traces = dot(send_pick, turned[...], 1, 1).astype(BF16)
    listed_traces = dot(listed_traces, narrow).astype(BF16)
    for p in range(cols):
        outgoing[p] = listed_traces[p * slots : (p + 1) * slots]

    face_copies = [face_copy(step) for step in range(1, cols)]
    for step in range(1, cols):
        if ordered:

            @pl.when((col + step >= cols) & (row % 2 == 0))
            def _():
                face_copies[step - 1].start()
        else:
            face_copies[step - 1].start()

    if ordered:
        later_sends(range(1, rows - 2), (row < 2) & (col > 0))
        later_sends(range(rows - 2, rows), row < 2)

    for copy in loads[1]:
        copy.wait()
    same_q = one_hot((vol_q, vol_q), lambda r, c: r == c)
    vol_basis = dot(same_q, vol_eval[...].astype(BF16), 1, 1).astype(BF16)
    for m in range(quantities):
        points[m] = dot(vol_basis, state_low[m])

    if ordered:
        for step in range(1, cols):

            @pl.when((col + step >= cols) & (row % 2 == 1))
            def _():
                face_copies[step - 1].start()

    if ordered:
        for step in range(1, cols):

            @pl.when(col + step < cols)
            def _():
                pl.semaphore_wait(col_in.at[step - 1], 1)
                face_copies[step - 1].start()

    elem_ids = lax.broadcasted_iota(jnp.int32, (elems, elems), 0).astype(F32).astype(BF16)
    one_low = jnp.ones((elems, elems), BF16)
    zero_low = jnp.zeros((elems, elems), BF16)
    for f in range(4):
        source = target[f : f + 1]
        near = kind[f : f + 1] == 0
        for g in range(4):
            hit = near & (source >= g * elems) & (source < (g + 1) * elems)
            wanted = jnp.where(hit, source - g * elems, -1).astype(F32).astype(BF16)
            pick[g * elems : (g + 1) * elems, :] = jnp.where(elem_ids == wanted, one_low, zero_low)
        gathered[:, f * elems : (f + 1) * elems] = dot(turned[...], pick[...])

    spread = one_hot(
        (4 * QP, 4 * face_q), lambda r, c: (c == (r % QP) * 4 + r // QP) & (r % QP < face_q)
    )
    for i in range(3):
        flat = normals[i].astype(F32).reshape(4 * face_q, elems).astype(BF16)
        normal_rows[i] = dot(spread, flat)
    flat = areas[...].reshape(4 * face_q, elems)
    high = flat.astype(BF16)
    low = (flat - high.astype(F32)).astype(BF16)
    area_rows[...] = dot(spread, high) + dot(spread, low)


    for t, steps in enumerate(groups):
        wide = len(steps) * unit

        def sent_point(k, c):
            step = steps[0] + c // unit
            sender = partner(row, step, rows) if direct else step
            return k == sender * unit + c % unit

        chosen_q = one_hot((vol_q, wide), sent_point)
        for d in range(3):
            at = tests_at[t] + d * wide
            tests[:, at : at + wide] = dot(vol_grad[d], chosen_q).astype(BF16)
    flat = face_lift[...].reshape(4 * face_q, basis).astype(BF16)
    place = one_hot(
        (4 * face_q, 4 * QP),
        lambda r, c: (r == (c % QP) * 4 + c // QP) & (c % QP < face_q),
    )
    at = tests_at[2]
    tests[:, at : at + 4 * QP] = (-dot(flat, place, 0, 0)).astype(BF16)

    lame = material[0:1, :]
    rigid = material[1:2, :]
    light = material[2:3, :]

    def volume_part(step, start, count, read):
        t = [step in steps for steps in groups].index(True)
        wide = len(groups[t]) * unit
        base = flux_at[t] + (step - groups[t][0]) * unit
        for half in range(elems // 128):
            cut = slice(half * 128, (half + 1) * 128)
            values = [points[m, pl.ds(start, count), cut] for m in range(9)]
            press = [-lame[:, cut] * values[6 + i] for i in range(3)]
            shear = [-rigid[:, cut] * values[6 + i] for i in range(3)]
            force = [-light[:, cut] * values[i] for i in range(6)]
            for d in range(3):
                n = [read(3 * d + i, cut) for i in range(3)]
                results = normal_flux(press, shear, force, n)
                at = base + d * wide
                for m in range(9):
                    fluxes[m, at : at + count, cut] = results[m].astype(BF16)

    def arrived(step):
        if step == 0:
            own_copy.wait()
        else:
            geo_copies[step].wait_recv()

    def volume(steps):
        if direct:
            for step in steps:
                arrived(step)
                sender = partner(row, step, rows)
                volume_part(
                    step,
                    pl.multiple_of(sender * local_q, local_q),
                    local_q,
                    lambda k, cut: metric[step, k, :, cut].astype(F32),
                )
        else:
            if steps[0] == 0:
                for step in range(rows):
                    arrived(step)
                    metric_by_row[partner(row, step, rows)] = metric[step].astype(F32)
            group = 16 // local_q
            for block in steps:
                volume_part(
                    block,
                    block * 16,
                    16,
                    lambda k, cut: jnp.concatenate(
                        [metric_by_row[block * group + j, k, :, cut] for j in range(group)], axis=0
                    ),
                )

    def contract(t, m):
        left = tests[:, tests_at[t] : tests_at[t] + depths[t]]
        return dot(left, fluxes[m, flux_at[t] : flux_at[t] + depths[t], :])

    pool_ids = lax.broadcasted_iota(jnp.int32, (cols * slots, elems), 0)
    for f in range(4):
        wanted = jnp.where(
            kind[f : f + 1] == 1, peer_index[f : f + 1] * slots + target[f : f + 1], -1
        )
        far[:, f * elems : (f + 1) * elems] = jnp.where(pool_ids == wanted, 1.0, 0.0).astype(BF16)
    own_speed = jnp.sqrt((lame + 2.0 * rigid) * light)

    def face_parts(f):
        for half in range(elems // 128):
            for part in range(QP // 16):
                yield slice(half * 128, (half + 1) * 128), f * QP + part * 16, part * 16

    def own_face(f):
        free = jnp.where(kind[f : f + 1] == 2, 1.0, 0.0)
        for cut, at, part in face_parts(f):
            a0, a1, a2 = -0.5 * lame[:, cut], -0.5 * rigid[:, cut], -0.5 * light[:, cut]
            n = [normal_rows[i, at : at + 16, cut] for i in range(3)]
            own = [traces[m, at : at + 16, cut] for m in range(9)]
            results = normal_flux(
                [a0 * own[6 + i] for i in range(3)],
                [a1 * own[6 + i] for i in range(3)],
                [a2 * own[i] for i in range(6)],
                n,
            )
            left = f * elems + cut.start
            for m in range(9):
                own_flux[m, at : at + 16, cut] = results[m]
                top = m * QP + part
                part_own = free[:, cut] * own[m]
                value = gathered[top : top + 16, left : left + 128]
                gathered[top : top + 16, left : left + 128] = (
                    value - part_own if m < 6 else value + part_own
                )

    def surface_face(f):
        lanes = slice(f * elems, (f + 1) * elems)
        edge = jnp.where(kind[f : f + 1] >= 2, 1.0, 0.0)
        other = []
        for i in range(3):
            high_at = i * QP + face_q
            low_at = (i + 3) * QP + face_q
            other.append(
                gathered[high_at : high_at + 1, lanes]
                + gathered[low_at : low_at + 1, lanes]
                + edge * material[i : i + 1, :]
            )
        speed = jnp.sqrt((other[0] + 2.0 * other[1]) * other[2])
        penalty_scale = 0.5 * jnp.maximum(own_speed, speed)
        for cut, at, part in face_parts(f):
            b0, b1, b2 = -0.5 * other[0][:, cut], -0.5 * other[1][:, cut], -0.5 * other[2][:, cut]
            n = [normal_rows[i, at : at + 16, cut] for i in range(3)]
            pen = penalty_scale[:, cut] * area_rows[at : at + 16, cut]
            left = f * elems + cut.start
            met = [gathered[m * QP + part : m * QP + part + 16, left : left + 128] for m in range(9)]
            results = normal_flux(
                [b0 * met[6 + i] for i in range(3)],
                [b1 * met[6 + i] for i in range(3)],
                [b2 * met[i] for i in range(6)],
                n,
            )
            to = flux_at[2] + at
            for m in range(9):
                gap = traces[m, at : at + 16, cut] - met[m]
                total = own_flux[m, at : at + 16, cut] + results[m] + pen * gap
                fluxes[m, to : to + 16, cut] = total.astype(BF16)

    factor = material[3:4, :]
    for f in range(4):
        own_face(f)
    volume(groups[0])
    for m in range(quantities):
        out[m] = contract(0, m)
    whole = pool.at[pl.ds(0, cols - 1)]
    pltpu.make_async_copy(whole, whole, face_recv).wait()
    received = pool[...].reshape(cols * slots, wire)
    received = dot(narrow, received, 1, 1).astype(BF16)
    gathered[...] = gathered[...] + dot(received, far[...])
    for f in range(4):
        surface_face(f)
    for m in range(quantities):
        out[m] = out[m] + contract(2, m)
    volume(groups[1])
    whole = metric.at[pl.ds(0, rows - 1)]
    pltpu.make_async_copy(whole, whole, geo_send).wait()
    whole = outgoing.at[pl.ds(0, cols - 1)]
    pltpu.make_async_copy(whole, whole, face_send).wait()
    for m in range(quantities):
        out[m] = state[m] + factor * (out[m] + contract(1, m))


def normal_flux(press, shear, force, n):
    pressure = press[0] * n[0] + press[1] * n[1] + press[2] * n[2]
    twice = [shear[i] + shear[i] for i in range(3)]
    return [
        pressure + twice[0] * n[0],
        pressure + twice[1] * n[1],
        pressure + twice[2] * n[2],
        n[0] * shear[1] + n[1] * shear[0],
        n[1] * shear[2] + n[2] * shear[1],
        n[0] * shear[2] + n[2] * shear[0],
        force[0] * n[0] + force[3] * n[1] + force[5] * n[2],
        force[3] * n[0] + force[1] * n[1] + force[4] * n[2],
        force[5] * n[0] + force[4] * n[1] + force[2] * n[2],
    ]


def per_device(
    rows,
    cols,
    state,
    geometry,
    material,
    neighbours,
    send_faces,
    vol_eval,
    vol_grad,
    face_eval,
    face_lift,
    normals,
    areas,
):
    quantities, basis, elems = state.shape
    slots = send_faces.shape[2]
    vol_q = vol_eval.shape[1]
    local_q = geometry.shape[1]
    total = 3 * vol_q + 4 * QP
    wire = (quantities * (face_eval.shape[2] + 1) + 127) // 128 * 128
    tests_at = tiles(vol_q, max(local_q, 16))[3]
    operands = [
        state,
        geometry,
        material,
        neighbours,
        send_faces,
        vol_eval,
        vol_grad,
        jnp.transpose(face_eval, (2, 0, 1)),
        jnp.transpose(face_lift, (2, 0, 1)),
        normals,
        areas,
    ]
    staged = [pltpu.VMEM(x.shape, x.dtype) for x in operands[:1] + operands[2:]]
    scratch = staged + [
        pltpu.VMEM((rows, 9, local_q, elems), BF16),
        pltpu.VMEM((quantities, basis, elems), BF16),
        pltpu.VMEM((quantities, 4 * QP, elems), F32),
        pltpu.VMEM((quantities * QP, 4 * elems), BF16),
        pltpu.VMEM((cols, slots, wire), BF16),
        pltpu.VMEM((cols, slots, wire), BF16),
        pltpu.VMEM((quantities * QP, 4 * elems), F32),
        pltpu.VMEM((quantities, vol_q, elems), F32),
        pltpu.VMEM((quantities, total, elems), BF16),
        pltpu.VMEM((basis, tests_at[-1]), BF16),
        pltpu.VMEM((3, 4 * QP, elems), F32),
        pltpu.VMEM((4 * QP, elems), F32),
        pltpu.VMEM((quantities, 4 * QP, elems), F32),
        pltpu.VMEM((4 * elems, elems), BF16),
        pltpu.VMEM((cols * slots, 4 * elems), BF16),
        pltpu.SemaphoreType.DMA((2,)),
        pltpu.SemaphoreType.DMA,
        pltpu.SemaphoreType.DMA((rows,)),
        pltpu.SemaphoreType.DMA,
        pltpu.SemaphoreType.DMA,
        pltpu.SemaphoreType.REGULAR((rows - 1,)),
        pltpu.SemaphoreType.REGULAR((cols - 1,)),
    ]
    if local_q % 16 != 0:
        scratch.append(pltpu.VMEM((rows, 9, local_q, elems), F32))
    return pl.pallas_call(
        functools.partial(kernel, rows, cols),
        out_shape=jax.ShapeDtypeStruct(state.shape, F32),
        in_specs=[pl.BlockSpec(memory_space=pltpu.HBM)] * len(operands),
        out_specs=pl.BlockSpec(memory_space=pltpu.VMEM),
        scratch_shapes=scratch,
        compiler_params=pltpu.CompilerParams(
            collective_id=0, has_side_effects=True, vmem_limit_bytes=48 * 1024 * 1024
        ),
    )(*[pltpu.with_memory_space_constraint(x, pltpu.HBM) for x in operands])


def solution(mesh):
    return jax.shard_map(
        functools.partial(per_device, mesh.shape["row"], mesh.shape["col"]),
        mesh=mesh,
        in_specs=(
            P(None, None, ("col", "row")),
            P(None, "row", "col"),
            P(None, ("col", "row")),
            P(None, None, ("col", "row")),
            P(("col", "row"), None, None),
            P(),
            P(),
            P(),
            P(),
            P(None, None, None, ("col", "row")),
            P(None, None, ("col", "row")),
        ),
        out_specs=P(None, None, ("col", "row")),
        check_vma=False,
    )
```
